32 devices in a mesh: dp: 4 (over y, z), tp: 8 (over x, core).
Axes of the slice: x: 4, y: 2, z: 2, core: 2. Of those that a mesh axis runs over, the one named last changes fastest.
The devices are a block of a 4x4x8 slice.
Arguments:
- hidden: bfloat16 [4, 16, 2048], P('dp'), parts along dimension 0
- norm_w: bfloat16 [2048], replicated
- embedding: bfloat16 [256000, 2048], P('tp')
- draft_ids: int32 [4, 16], P('dp'), parts along dimension 0
Outputs:
- output 1: float32 [4, 16], P('dp'), parts along dimension 0
- output 2: float32 [4, 16], P('dp'), parts along dimension 0
There are 4 independent parts. The reference program is written for one: setup_inputs(seed, part) draws one part's arguments, and reference() takes and returns one part's arrays. A program takes and returns all parts, laid end to end along the dimension named above; an argument that names none is the same for every part.
All inputs are finite; a program needn't handle non-finite values.
Results may differ from the reference program's by a relative error of at most 0.001.
Values sent between devices are 32-bit elements.
A program may use at most 768 MiB of HBM per device.

```python
import jax
import jax.numpy as jnp
from jax import lax

BATCH = 1
DRAFT = 16
D = 2048
VOCAB = 256000
EPS = 1e-6
ROW_BLOCK = 2 ** 11
HOT_IDS = VOCAB // 16
ALIGN_SCALE = 6.0
NOISE_SCALE = 3.0


def draw_embedding(key_coef, key_noise, direction):
    num_blocks = VOCAB // ROW_BLOCK

    def one_block(block_idx):
        tok_coef = jax.random.normal(jax.random.fold_in(key_coef, block_idx), (ROW_BLOCK, 1), jnp.float32)
        noise_rows = jax.random.normal(jax.random.fold_in(key_noise, block_idx), (ROW_BLOCK, D), jnp.float32)
        block_rows = ALIGN_SCALE * tok_coef * direction / D + NOISE_SCALE * noise_rows * D ** -0.5
        return block_rows.astype(jnp.bfloat16)

    return lax.map(one_block, jnp.arange(num_blocks)).reshape(VOCAB, D)


def setup_inputs(seed: int = 0, part: int = 0) -> dict:
    base_key = jax.random.key(seed)
    key_dir, key_w, key_coef, key_noise, key_part = jax.random.split(base_key, 5)
    key_part = jax.random.fold_in(key_part, part)
    key_mix, key_hid, key_pick, key_low, key_any = jax.random.split(key_part, 5)
    direction = jax.random.normal(key_dir, (D,), jnp.float32)
    mix_coef = jax.random.uniform(key_mix, (BATCH, DRAFT, 1), jnp.float32, -0.9, 0.9)
    hid_noise = jax.random.normal(key_hid, (BATCH, DRAFT, D), jnp.float32)
    hidden = mix_coef * direction + jnp.sqrt(1.0 - mix_coef * mix_coef) * hid_noise
    norm_w = 0.5 * jax.random.normal(key_w, (D,), jnp.float32)
    embedding = draw_embedding(key_coef, key_noise, direction)
    pick_kind = jax.random.randint(key_pick, (BATCH, DRAFT), 0, 4)
    low_ids = jax.random.randint(key_low, (BATCH, DRAFT), 0, HOT_IDS)
    any_ids = jax.random.randint(key_any, (BATCH, DRAFT), 0, VOCAB)
    draft_ids = jnp.where(pick_kind < 3, low_ids, any_ids).astype(jnp.int32)
    draft_ids = draft_ids.at[0, 0].set(VOCAB - 1).at[0, 1].set(0)
    return {"hidden": hidden.astype(jnp.bfloat16), "norm_w": norm_w.astype(jnp.bfloat16), "embedding": embedding, "draft_ids": draft_ids}


def reference(hidden, norm_w, embedding, draft_ids):
    gain = 1.0 + norm_w.astype(jnp.float32)

    def one_seq(seq_args):
        seq_hidden, seq_ids = seq_args
        x_float = seq_hidden.astype(jnp.float32)
        mean_sq = jnp.mean(x_float * x_float, axis=-1, keepdims=True)
        normed = (x_float * lax.rsqrt(mean_sq + EPS) * gain).astype(jnp.bfloat16)
        logits = jnp.dot(normed, embedding.T, preferred_element_type=jnp.float32)
        row_max = jnp.max(logits, axis=-1, keepdims=True)
        exp_shift = jnp.exp(logits - row_max)
        exp_total = jnp.sum(exp_shift, axis=-1)
        weighted = jnp.sum(exp_shift * logits, axis=-1)
        log_norm = row_max[:, 0] + jnp.log(exp_total)
        picked = jnp.take_along_axis(logits, seq_ids[:, None], axis=-1)[:, 0]
        return picked - log_norm, log_norm - weighted / exp_total

    log_prob, entropy = lax.map(one_seq, (hidden, draft_ids))
    return log_prob, entropy
```

```python
import functools

import jax
import jax.numpy as jnp
from jax import lax
from jax.experimental import pallas as pl
from jax.experimental.pallas import tpu as pltpu
from jax.sharding import PartitionSpec as P

EPS = 1e-6
MESH = pl.DeviceIdType.MESH
LANES = 128
HALVES = 2
SHARE = 4
CHUNK_ROWS = 800


def head_kernel(
    group, tp, rows, hid_hbm, w_hbm, emb_hbm, ids_hbm, lp_ref, ent_ref,
    hid_v, w_v, ids_v, hx, ids_x, hb, ebuf, zs, sbuf, rbuf,
    in_sem, esem, h_send, h_recv, f_send, f_recv, id_send, id_recv, s_send, s_recv,
):
    npos, depth = hid_v.shape
    half = depth // HALVES
    chunk = CHUNK_ROWS
    nchunk = rows // chunk
    nsrc = group * tp

    dp_me = lax.axis_index("dp")
    tp_me = lax.axis_index("tp")
    q = lax.rem(dp_me, group)
    base = dp_me - q
    c = lax.rem(tp_me, 2)
    sibling = tp_me + 1 - 2 * c
    me = q * tp + tp_me

    def peer(r):
        return base + lax.rem(q + r, group)

    small = [
        pltpu.make_async_copy(hid_hbm.at[0], hid_v, in_sem.at[0]),
        pltpu.make_async_copy(w_hbm, w_v, in_sem.at[1]),
        pltpu.make_async_copy(ids_hbm, ids_v, in_sem.at[2]),
    ]
    for copy in small:
        copy.start()
    loads = []
    for j in range(nchunk):
        pair = []
        for o in range(HALVES):
            col = half * (c if o == 0 else 1 - c)
            copy = pltpu.make_async_copy(
                emb_hbm.at[pl.ds(q * rows + j * chunk, chunk), pl.ds(pl.multiple_of(col, half), half)],
                ebuf.at[o, pl.ds(j * chunk, chunk)],
                esem.at[j, o],
            )
            copy.start()
            pair.append(copy)
        loads.append(pair)

    barrier = pltpu.get_barrier_semaphore()
    for r in range(group):
        for t in range(tp):
            if r or t:
                pl.semaphore_signal(
                    barrier, inc=1, device_id=(peer(r), lax.rem(tp_me + t, tp)), device_id_type=MESH
                )

    for copy in small:
        copy.wait()
    x = hid_v[...].astype(jnp.float32)
    scale = lax.rsqrt(jnp.mean(x * x, axis=-1, keepdims=True) + EPS)
    h = (x * scale * (1.0 + w_v[...].astype(jnp.float32))).astype(jnp.bfloat16)
    h32 = h.astype(jnp.float32)
    for s in range(HALVES):
        hx[q, s] = h32[:, s * half:(s + 1) * half]
    ids_x[q] = jnp.concatenate([ids_v[...], jnp.full((1, LANES - npos), -1, jnp.int32)], axis=1)

    pl.semaphore_wait(barrier, nsrc - 1)

    direct, ident = [], []
    for r in range(1, group):
        copy = pltpu.make_async_remote_copy(
            src_ref=hx.at[q, c], dst_ref=hx.at[q, c], send_sem=h_send.at[r], recv_sem=h_recv.at[r],
            device_id=(peer(r), tp_me), device_id_type=MESH)
        copy.start()
        direct.append(copy)
    for r in range(1, group):
        copy = pltpu.make_async_remote_copy(
            src_ref=ids_x.at[q], dst_ref=ids_x.at[q], send_sem=id_send.at[r], recv_sem=id_recv.at[r],
            device_id=(peer(r), tp_me), device_id_type=MESH)
        copy.start()
        ident.append(copy)

    def place(p, o):
        col = c if o == 0 else 1 - c
        hb[o, pl.ds(pl.multiple_of(p * npos, npos), npos), :] = hx[p, col].astype(jnp.bfloat16)

    for o in range(HALVES):
        place(q, o)
    forward = []
    for r in range(1, group):
        p = lax.rem(q - r + group, group)
        direct[r - 1].wait_recv()
        copy = pltpu.make_async_remote_copy(
            src_ref=hx.at[p, c], dst_ref=hx.at[p, c], send_sem=f_send.at[r], recv_sem=f_recv.at[r],
            device_id=(dp_me, sibling), device_id_type=MESH)
        copy.start()
        forward.append(copy)
        place(p, 0)
    for copy in ident:
        copy.wait_recv()

    lane = lax.broadcasted_iota(jnp.int32, (8, LANES), 1)
    want = jnp.full((8, LANES), -1, jnp.int32)
    for p in range(group):
        moved = jnp.broadcast_to(ids_x[p], (8, LANES))
        if p:
            moved = pltpu.roll(moved, p * npos, 1)
        want = jnp.where((lane >= p * npos) & (lane < (p + 1) * npos), moved, want)
    first_row = tp_me * (rows * group) + q * rows
    want = want - first_row - lax.broadcasted_iota(jnp.int32, (8, LANES), 0)

    def score(j, o):
        return lax.dot_general(
            ebuf[o, j * chunk:(j + 1) * chunk, :], hb[o], (((1,), (1,)), ((), ())), preferred_element_type=jnp.float32)

    def stats(j, state):
        z = zs[j % 2].reshape(chunk // 8, 8, LANES)
        top = jnp.max(z, axis=0)
        row = lax.broadcasted_iota(jnp.int32, (chunk // 8, 8, LANES), 0) * 8 + j * chunk
        pick = jnp.sum(jnp.where(row == want[None], z, 0.0), axis=0)
        if state is not None:
            top = jnp.maximum(top, state[0])
        e = jnp.exp(z - top[None])
        total = jnp.sum(e, axis=0)
        weighted = jnp.sum(e * z, axis=0)
        if state is not None:
            fade = jnp.exp(state[0] - top)
            total = total + state[1] * fade
            weighted = weighted + state[2] * fade
            pick = pick + state[3]
        return top, total, weighted, pick

    for s in range(2):
        zs[s] = jnp.zeros((chunk, LANES), jnp.float32)
    state = None
    for j in range(nchunk):
        loads[j][0].wait()
        if j == 0:
            first = score(0, 0)
            for r in range(1, group):
                forward[r - 1].wait_recv()
                place(lax.rem(q - r + group, group), 1)
            loads[0][1].wait()
            zs[0, :, :group * npos] = first + score(0, 1)
        else:
            loads[j][1].wait()
            zs[j % 2, :, :group * npos] = score(j, 0) + score(j, 1)
            state = stats(j - 1, state)
    state = stats(nchunk - 1, state)

    top8, total8, weighted8, pick8 = state
    top = jnp.max(top8, axis=0, keepdims=True)
    fade = jnp.exp(top8 - top)
    full = lambda v: jnp.broadcast_to(v, (8, LANES))
    top = full(top)
    total = full(jnp.sum(total8 * fade, axis=0, keepdims=True))
    weighted = full(jnp.sum(weighted8 * fade, axis=0, keepdims=True))
    pick = full(jnp.sum(pick8, axis=0, keepdims=True))
    for p in range(group):
        message = jnp.zeros((8, LANES), jnp.float32)
        for at, v in ((0, top), (1, top), (4, total), (5, weighted), (6, pick)):
            shift = (at * npos - p * npos) % LANES
            moved = pltpu.roll(v, shift, 1) if shift else v
            message = jnp.where((lane >= at * npos) & (lane < (at + 1) * npos), moved, message)
        sbuf[p] = message[:1]

    for r in range(group):
        for t in range(tp):
            if r or t:
                pltpu.make_async_remote_copy(
                    src_ref=sbuf.at[lax.rem(q + r, group)], dst_ref=rbuf.at[me], send_sem=s_send, recv_sem=s_recv,
                    device_id=(peer(r), lax.rem(tp_me + t, tp)), device_id_type=MESH).start()
    rbuf[me] = sbuf[q]
    for copies in (direct, ident, forward):
        for copy in copies:
            copy.wait_send()
    everyone = pltpu.make_async_remote_copy(
        src_ref=rbuf.at[pl.ds(0, nsrc - 1)], dst_ref=rbuf.at[pl.ds(0, nsrc - 1)], send_sem=s_send, recv_sem=s_recv,
        device_id=(dp_me, tp_me), device_id_type=MESH)
    everyone.wait_recv()
    everyone.wait_send()

    got = rbuf[...]
    values = pltpu.roll(got, LANES // 2, 2)
    top = jnp.max(got, axis=0)
    sums = jnp.sum(jnp.exp(got - top[None]) * values, axis=0)
    total = sums[:, :npos]
    weighted = pltpu.roll(sums, LANES - npos, 1)[:, :npos]
    pick = pltpu.roll(sums, LANES - 2 * npos, 1)[:, :npos]
    log_norm = top[:, :npos] + jnp.log(total)
    lp_ref[...] = pick - log_norm
    ent_ref[...] = log_norm - weighted / total


def solution(mesh):
    tp = mesh.shape["tp"]
    group = next(n for n in (SHARE, 2, 1) if mesh.shape["dp"] % n == 0)

    def local_part(hidden, norm_w, embedding, draft_ids):
        npos, depth = hidden.shape[1:]
        rows = embedding.shape[0] // group
        half = depth // HALVES
        nchunk = rows // CHUNK_ROWS
        any_spec = pl.BlockSpec(memory_space=pl.ANY)
        dma = pltpu.SemaphoreType.DMA
        return pl.pallas_call(
            functools.partial(head_kernel, group, tp, rows),
            out_shape=[jax.ShapeDtypeStruct((1, npos), jnp.float32)] * 2,
            in_specs=[any_spec] * 4,
            out_specs=[pl.BlockSpec(memory_space=pltpu.VMEM)] * 2,
            scratch_shapes=[
                pltpu.VMEM((npos, depth), jnp.bfloat16),
                pltpu.VMEM((1, depth), jnp.bfloat16),
                pltpu.VMEM((1, npos), jnp.int32),
                pltpu.VMEM((group, HALVES, npos, half), jnp.float32),
                pltpu.VMEM((group, 1, LANES), jnp.int32),
                pltpu.VMEM((HALVES, group * npos, half), jnp.bfloat16),
                pltpu.VMEM((HALVES, rows, half), jnp.bfloat16),
                pltpu.VMEM((2, CHUNK_ROWS, LANES), jnp.float32),
                pltpu.VMEM((group, 1, LANES), jnp.float32),
                pltpu.VMEM((group * tp, 1, LANES), jnp.float32),
                dma((3,)), dma((nchunk, HALVES)),
                dma((group,)), dma((group,)), dma((group,)), dma((group,)), dma((group,)), dma((group,)),
                dma, dma,
            ],
            compiler_params=pltpu.CompilerParams(
                collective_id=0, has_side_effects=True, vmem_limit_bytes=60 * 2**20),
        )(hidden, norm_w.reshape(1, depth), embedding, draft_ids)

    return jax.shard_map(
        local_part, mesh=mesh,
        in_specs=(P("dp", None, None), P(None), P("tp", None), P("dp", None)),
        out_specs=(P("dp", None), P("dp", None)), check_vma=False)
```

```python
import functools

import jax
import jax.numpy as jnp
from jax import lax
from jax.experimental import pallas as pl
from jax.experimental.pallas import tpu as pltpu
from jax.sharding import PartitionSpec as P

EPS = 1e-6
MESH = pl.DeviceIdType.MESH
LANES = 128
HALVES = 2
SHARE = 4
CHUNK_ROWS = 800
PARTS = 2


def head_kernel(
    group, tp, rows, hid_hbm, w_hbm, emb_hbm, ids_hbm, got_ref,
    hid_v, w_v, ids_v, hx, ids_x, hb, ebuf, zs, sbuf, rbuf,
    in_sem, esem, h_send, h_recv, f_send, f_recv, id_send, id_recv, s_send, s_recv,
):
    npos, depth = hid_v.shape
    half = depth // HALVES
    chunk = CHUNK_ROWS
    nchunk = rows // chunk
    nsrc = group * tp

    dp_me = lax.axis_index("dp")
    tp_me = lax.axis_index("tp")
    q = lax.rem(dp_me, group)
    base = dp_me - q
    c = lax.rem(tp_me, 2)
    sibling = tp_me + 1 - 2 * c
    me = q * tp + tp_me

    def peer(r):
        return base + lax.rem(q + r, group)

    small = [
        pltpu.make_async_copy(hid_hbm.at[0], hid_v, in_sem.at[0]),
        pltpu.make_async_copy(w_hbm, w_v, in_sem.at[1]),
        pltpu.make_async_copy(ids_hbm, ids_v, in_sem.at[2]),
    ]
    for copy in small:
        copy.start()
    loads = []
    for j in range(nchunk):
        pair = []
        for o in range(HALVES):
            col = half * (c if o == 0 else 1 - c)
            copy = pltpu.make_async_copy(
                emb_hbm.at[pl.ds(q * rows + j * chunk, chunk), pl.ds(pl.multiple_of(col, half), half)],
                ebuf.at[pl.ds(j * chunk, chunk), pl.ds(o * half, half)],
                esem.at[j, o],
            )
            copy.start()
            pair.append(copy)
        loads.append(pair)

    barrier = pltpu.get_barrier_semaphore()
    for r in range(group):
        for t in range(tp):
            if r or t:
                pl.semaphore_signal(
                    barrier, inc=1, device_id=(peer(r), lax.rem(tp_me + t, tp)), device_id_type=MESH
                )

    for copy in small:
        copy.wait()
    x = hid_v[...].astype(jnp.float32)
    scale = lax.rsqrt(jnp.mean(x * x, axis=-1, keepdims=True) + EPS)
    h = (x * scale * (1.0 + w_v[...].astype(jnp.float32).reshape(1, depth))).astype(jnp.bfloat16)
    h32 = h.astype(jnp.float32)
    for s in range(HALVES):
        hx[q, s] = h32[:, s * half:(s + 1) * half]
    ids_x[q] = jnp.concatenate([ids_v[...], jnp.full((1, LANES - npos), -1, jnp.int32)], axis=1)

    pl.semaphore_wait(barrier, nsrc - 1)

    direct, ident = [], []
    for r in range(1, group):
        copy = pltpu.make_async_remote_copy(
            src_ref=hx.at[q, c], dst_ref=hx.at[q, c], send_sem=h_send.at[r], recv_sem=h_recv.at[r],
            device_id=(peer(r), tp_me), device_id_type=MESH)
        copy.start()
        direct.append(copy)
    for r in range(1, group):
        copy = pltpu.make_async_remote_copy(
            src_ref=ids_x.at[q], dst_ref=ids_x.at[q], send_sem=id_send.at[r], recv_sem=id_recv.at[r],
            device_id=(peer(r), tp_me), device_id_type=MESH)
        copy.start()
        ident.append(copy)

    def place(p, o):
        col = c if o == 0 else 1 - c
        hb[pl.ds(pl.multiple_of(p * npos, npos), npos), o * half:(o + 1) * half] = hx[p, col].astype(jnp.bfloat16)

    for o in range(HALVES):
        place(q, o)
    forward = []
    for r in range(1, group):
        p = lax.rem(q - r + group, group)
        direct[r - 1].wait_recv()
        copy = pltpu.make_async_remote_copy(
            src_ref=hx.at[p, c], dst_ref=hx.at[p, c], send_sem=f_send.at[r], recv_sem=f_recv.at[r],
            device_id=(dp_me, sibling), device_id_type=MESH)
        copy.start()
        forward.append(copy)
        place(p, 0)
    for copy in ident:
        copy.wait_recv()

    lane = lax.broadcasted_iota(jnp.int32, (8, LANES), 1)
    want = jnp.full((8, LANES), -1, jnp.int32)
    for p in range(group):
        moved = jnp.broadcast_to(ids_x[p], (8, LANES))
        if p:
            moved = pltpu.roll(moved, p * npos, 1)
        want = jnp.where((lane >= p * npos) & (lane < (p + 1) * npos), moved, want)
    first_row = tp_me * (rows * group) + q * rows
    want = want - first_row - lax.broadcasted_iota(jnp.int32, (8, LANES), 0)

    def score(j, lo, hi):
        out = []
        for m in range(PARTS):
            first = j * chunk + m * (chunk // PARTS)
            out.append(lax.dot_general(
                ebuf[first:first + chunk // PARTS, lo:hi], hb[:, lo:hi], (((1,), (1,)), ((), ())),
                preferred_element_type=jnp.float32))
        return out

    def keep(j, parts):
        for m, part in enumerate(parts):
            n = chunk // PARTS
            zs[j % 2, m * n:(m + 1) * n, :group * npos] = part

    def stats(j, state):
        z = zs[j % 2].reshape(chunk // 8, 8, LANES)
        top = jnp.max(z, axis=0)
        row = lax.broadcasted_iota(jnp.int32, (chunk // 8, 8, LANES), 0) * 8 + j * chunk
        pick = jnp.sum(jnp.where(row == want[None], z, 0.0), axis=0)
        if state is not None:
            top = jnp.maximum(top, state[0])
        e = jnp.exp(z - top[None])
        total = jnp.sum(e, axis=0)
        weighted = jnp.sum(e * z, axis=0)
        if state is not None:
            fade = jnp.exp(state[0] - top)
            total = total + state[1] * fade
            weighted = weighted + state[2] * fade
            pick = pick + state[3]
        return top, total, weighted, pick

    for s in range(2):
        zs[s] = jnp.zeros((chunk, LANES), jnp.float32)
    state = None
    for j in range(nchunk):
        loads[j][0].wait()
        if j == 0:
            first = score(0, 0, half)
            for r in range(1, group):
                forward[r - 1].wait_recv()
                place(lax.rem(q - r + group, group), 1)
            loads[0][1].wait()
            keep(0, [u + v for u, v in zip(first, score(0, half, depth))])
        else:
            loads[j][1].wait()
            keep(j, score(j, 0, depth))
            state = stats(j - 1, state)
    state = stats(nchunk - 1, state)

    top8, total8, weighted8, pick8 = state
    top = jnp.max(top8, axis=0, keepdims=True)
    fade = jnp.exp(top8 - top)
    full = lambda v: jnp.broadcast_to(v, (8, LANES))
    top = full(top)
    total = full(jnp.sum(total8 * fade, axis=0, keepdims=True))
    weighted = full(jnp.sum(weighted8 * fade, axis=0, keepdims=True))
    pick = full(jnp.sum(pick8, axis=0, keepdims=True))
    for p in range(group):
        message = jnp.zeros((8, LANES), jnp.float32)
        for at, v in ((0, top), (1, top), (4, total), (5, weighted), (6, pick)):
            shift = (at * npos - p * npos) % LANES
            moved = pltpu.roll(v, shift, 1) if shift else v
            message = jnp.where((lane >= at * npos) & (lane < (at + 1) * npos), moved, message)
        sbuf[p] = message[:1]

    for r in range(group):
        for t in range(tp):
            if r or t:
                pltpu.make_async_remote_copy(
                    src_ref=sbuf.at[lax.rem(q + r, group)], dst_ref=rbuf.at[me], send_sem=s_send, recv_sem=s_recv,
                    device_id=(peer(r), lax.rem(tp_me + t, tp)), device_id_type=MESH).start()
    rbuf[me] = sbuf[q]
    for copies in (direct, ident, forward):
        for copy in copies:
            copy.wait_send()
    everyone = pltpu.make_async_remote_copy(
        src_ref=rbuf.at[pl.ds(0, nsrc - 1)], dst_ref=rbuf.at[pl.ds(0, nsrc - 1)], send_sem=s_send, recv_sem=s_recv,
        device_id=(dp_me, tp_me), device_id_type=MESH)
    everyone.wait_recv()
    everyone.wait_send()

    got_ref[...] = rbuf[...]


def combine_kernel(npos, got_ref, lp_ref, ent_ref):
    got = got_ref[...]
    values = pltpu.roll(got, LANES // 2, 2)
    top = jnp.max(got, axis=0)
    sums = jnp.sum(jnp.exp(got - top[None]) * values, axis=0)
    total = sums[:, :npos]
    weighted = pltpu.roll(sums, LANES - npos, 1)[:, :npos]
    pick = pltpu.roll(sums, LANES - 2 * npos, 1)[:, :npos]
    log_norm = top[:, :npos] + jnp.log(total)
    lp_ref[...] = pick - log_norm
    ent_ref[...] = log_norm - weighted / total


def solution(mesh):
    tp = mesh.shape["tp"]
    group = next(n for n in (SHARE, 2, 1) if mesh.shape["dp"] % n == 0)

    def local_part(hidden, norm_w, embedding, draft_ids):
        npos, depth = hidden.shape[1:]
        rows = embedding.shape[0] // group
        half = depth // HALVES
        nchunk = rows // CHUNK_ROWS
        any_spec = pl.BlockSpec(memory_space=pl.ANY)
        dma = pltpu.SemaphoreType.DMA
        got = pl.pallas_call(
            functools.partial(head_kernel, group, tp, rows),
            out_shape=jax.ShapeDtypeStruct((group * tp, 1, LANES), jnp.float32),
            in_specs=[any_spec] * 4,
            out_specs=pl.BlockSpec(memory_space=pltpu.VMEM),
            scratch_shapes=[
                pltpu.VMEM((npos, depth), jnp.bfloat16),
                pltpu.VMEM((depth,), jnp.bfloat16),
                pltpu.VMEM((1, npos), jnp.int32),
                pltpu.VMEM((group, HALVES, npos, half), jnp.float32),
                pltpu.VMEM((group, 1, LANES), jnp.int32),
                pltpu.VMEM((group * npos, depth), jnp.bfloat16),
                pltpu.VMEM((rows, depth), jnp.bfloat16),
                pltpu.VMEM((2, CHUNK_ROWS, LANES), jnp.float32),
                pltpu.VMEM((group, 1, LANES), jnp.float32),
                pltpu.VMEM((group * tp, 1, LANES), jnp.float32),
                dma((3,)), dma((nchunk, HALVES)),
                dma((group,)), dma((group,)), dma((group,)), dma((group,)), dma((group,)), dma((group,)),
                dma, dma,
            ],
            compiler_params=pltpu.CompilerParams(
                collective_id=0, has_side_effects=True, vmem_limit_bytes=60 * 2**20),
        )(hidden, norm_w, embedding, draft_ids)
        return pl.pallas_call(
            functools.partial(combine_kernel, npos),
            out_shape=[jax.ShapeDtypeStruct((1, npos), jnp.float32)] * 2,
            in_specs=[pl.BlockSpec(memory_space=pltpu.VMEM)],
            out_specs=[pl.BlockSpec(memory_space=pltpu.VMEM)] * 2,
        )(got)

    return jax.shard_map(
        local_part, mesh=mesh,
        in_specs=(P("dp", None, None), P(None), P("tp", None), P("dp", None)),
        out_specs=(P("dp", None), P("dp", None)), check_vma=False)
```

```python
import functools

import jax
import jax.numpy as jnp
from jax import lax
from jax.experimental import pallas as pl
from jax.experimental.pallas import tpu as pltpu
from jax.sharding import PartitionSpec as P

EPS = 1e-6
MESH = pl.DeviceIdType.MESH
LANES = 128
HALVES = 2
SHARE = 4
CHUNK_ROWS = 800
PARTS = 2
BEFORE_BARRIER = 2
BEFORE_FORWARD = 5
BLOCKS = (4, 99)


def head_kernel(
    group, tp, rows, hid_hbm, w_hbm, emb_hbm, ids_hbm, got_ref,
    hid_v, w_v, ids_v, hx, ids_x, hb, ebuf, zs, sbuf, rbuf,
    in_sem, esem, h_send, h_recv, f_send, f_recv, id_send, id_recv, s_send, s_recv,
):
    npos, depth = hid_v.shape
    half = depth // HALVES
    chunk = CHUNK_ROWS
    nchunk = rows // chunk
    nsrc = group * tp

    dp_me = lax.axis_index("dp")
    tp_me = lax.axis_index("tp")
    q = lax.rem(dp_me, group)
    base = dp_me - q
    c = lax.rem(tp_me, 2)
    sibling = tp_me + 1 - 2 * c
    me = q * tp + tp_me

    def peer(r):
        return base + lax.rem(q + r, group)

    small = [
        pltpu.make_async_copy(hid_hbm.at[0], hid_v, in_sem.at[0]),
        pltpu.make_async_copy(w_hbm, w_v, in_sem.at[1]),
        pltpu.make_async_copy(ids_hbm, ids_v, in_sem.at[2]),
    ]
    for copy in small:
        copy.start()
    loads = []
    for j in range(nchunk):
        for o in range(HALVES):
            col = half * (c if o == 0 else 1 - c)
            loads.append(pltpu.make_async_copy(
                emb_hbm.at[pl.ds(q * rows + j * chunk, chunk), pl.ds(pl.multiple_of(col, half), half)],
                ebuf.at[pl.ds(j * chunk, chunk), pl.ds(o * half, half)],
                esem.at[j, o],
            ))

    def fetch(lo, hi):
        for copy in loads[lo * HALVES:hi * HALVES]:
            copy.start()

    def arrive(lo, hi):
        for copy in loads[lo * HALVES:hi * HALVES]:
            copy.wait()

    fetch(0, BEFORE_BARRIER)

    barrier = pltpu.get_barrier_semaphore()
    for r in range(group):
        for t in range(tp):
            if r or t:
                pl.semaphore_signal(
                    barrier, inc=1, device_id=(peer(r), lax.rem(tp_me + t, tp)), device_id_type=MESH
                )

    for copy in small:
        copy.wait()
    x = hid_v[...].astype(jnp.float32)
    scale = lax.rsqrt(jnp.mean(x * x, axis=-1, keepdims=True) + EPS)
    h = (x * scale * (1.0 + w_v[...].astype(jnp.float32).reshape(1, depth))).astype(jnp.bfloat16)
    h32 = h.astype(jnp.float32)
    for s in range(HALVES):
        hx[q, s] = h32[:, s * half:(s + 1) * half]
    ids_x[q] = jnp.concatenate([ids_v[...], jnp.full((1, LANES - npos), -1, jnp.int32)], axis=1)

    zs[:, :, group * npos:] = jnp.zeros((nchunk, chunk, LANES - group * npos), jnp.float32)
    pl.semaphore_wait(barrier, nsrc - 1)

    direct, ident = [], []
    for r in range(1, group):
        copy = pltpu.make_async_remote_copy(
            src_ref=hx.at[q, c], dst_ref=hx.at[q, c], send_sem=h_send.at[r], recv_sem=h_recv.at[r],
            device_id=(peer(r), tp_me), device_id_type=MESH)
        copy.start()
        direct.append(copy)
    for r in range(1, group):
        copy = pltpu.make_async_remote_copy(
            src_ref=ids_x.at[q], dst_ref=ids_x.at[q], send_sem=id_send.at[r], recv_sem=id_recv.at[r],
            device_id=(peer(r), tp_me), device_id_type=MESH)
        copy.start()
        ident.append(copy)
    fetch(BEFORE_BARRIER, BEFORE_FORWARD)

    def place(p, o):
        col = c if o == 0 else 1 - c
        hb[pl.ds(pl.multiple_of(p * npos, npos), npos), o * half:(o + 1) * half] = hx[p, col].astype(jnp.bfloat16)

    for o in range(HALVES):
        place(q, o)
    forward = []
    for r in range(1, group):
        p = lax.rem(q - r + group, group)
        direct[r - 1].wait_recv()
        copy = pltpu.make_async_remote_copy(
            src_ref=hx.at[p, c], dst_ref=hx.at[p, c], send_sem=f_send.at[r], recv_sem=f_recv.at[r],
            device_id=(dp_me, sibling), device_id_type=MESH)
        copy.start()
        forward.append(copy)
        place(p, 0)
    fetch(BEFORE_FORWARD, nchunk)
    for copy in ident:
        copy.wait_recv()

    lane = lax.broadcasted_iota(jnp.int32, (8, LANES), 1)
    want = jnp.full((8, LANES), -1, jnp.int32)
    for p in range(group):
        moved = jnp.broadcast_to(ids_x[p], (8, LANES))
        if p:
            moved = pltpu.roll(moved, p * npos, 1)
        want = jnp.where((lane >= p * npos) & (lane < (p + 1) * npos), moved, want)
    first_row = tp_me * (rows * group) + q * rows
    want = want - first_row - lax.broadcasted_iota(jnp.int32, (8, LANES), 0)

    def score(j, lo, hi):
        out = []
        for m in range(PARTS):
            first = j * chunk + m * (chunk // PARTS)
            out.append(lax.dot_general(
                ebuf[first:first + chunk // PARTS, lo:hi], hb[:, lo:hi], (((1,), (1,)), ((), ())),
                preferred_element_type=jnp.float32))
        return out

    def keep(j, parts):
        for m, part in enumerate(parts):
            n = chunk // PARTS
            zs[j, m * n:(m + 1) * n, :group * npos] = part

    def stats(j, state):
        z = zs[j].reshape(chunk // 8, 8, LANES)
        top = jnp.max(z, axis=0)
        row = lax.broadcasted_iota(jnp.int32, (chunk // 8, 8, LANES), 0) * 8 + j * chunk
        pick = jnp.sum(jnp.where(row == want[None], z, 0.0), axis=0)
        if state is not None:
            top = jnp.maximum(top, state[0])
        e = jnp.exp(z - top[None])
        total = jnp.sum(e, axis=0)
        weighted = jnp.sum(e * z, axis=0)
        if state is not None:
            fade = jnp.exp(state[0] - top)
            total = total + state[1] * fade
            weighted = weighted + state[2] * fade
            pick = pick + state[3]
        return top, total, weighted, pick

    loads[0].wait()
    first = score(0, 0, half)
    for r in range(1, group):
        forward[r - 1].wait_recv()
        place(lax.rem(q - r + group, group), 1)
    loads[1].wait()
    keep(0, [u + v for u, v in zip(first, score(0, half, depth))])
    state = None
    at = 1
    for size in BLOCKS:
        end = min(at + size, nchunk)
        arrive(at, end)
        for j in range(at, end):
            keep(j, score(j, 0, depth))
            state = stats(j - 1, state)
        at = end
    state = stats(nchunk - 1, state)

    top8, total8, weighted8, pick8 = state
    top = jnp.max(top8, axis=0, keepdims=True)
    fade = jnp.exp(top8 - top)
    full = lambda v: jnp.broadcast_to(v, (8, LANES))
    top = full(top)
    total = full(jnp.sum(total8 * fade, axis=0, keepdims=True))
    weighted = full(jnp.sum(weighted8 * fade, axis=0, keepdims=True))
    pick = full(jnp.sum(pick8, axis=0, keepdims=True))
    for p in range(group):
        message = jnp.zeros((8, LANES), jnp.float32)
        for at, v in ((0, top), (1, top), (4, total), (5, weighted), (6, pick)):
            shift = (at * npos - p * npos) % LANES
            moved = pltpu.roll(v, shift, 1) if shift else v
            message = jnp.where((lane >= at * npos) & (lane < (at + 1) * npos), moved, message)
        sbuf[p] = message[:1]

    for r in range(group):
        for t in range(tp):
            if r or t:
                pltpu.make_async_remote_copy(
                    src_ref=sbuf.at[lax.rem(q + r, group)], dst_ref=rbuf.at[me], send_sem=s_send, recv_sem=s_recv,
                    device_id=(peer(r), lax.rem(tp_me + t, tp)), device_id_type=MESH).start()
    rbuf[me] = sbuf[q]
    for copies in (direct, ident, forward):
        for copy in copies:
            copy.wait_send()
    everyone = pltpu.make_async_remote_copy(
        src_ref=rbuf.at[pl.ds(0, nsrc - 1)], dst_ref=rbuf.at[pl.ds(0, nsrc - 1)], send_sem=s_send, recv_sem=s_recv,
        device_id=(dp_me, tp_me), device_id_type=MESH)
    everyone.wait_recv()
    everyone.wait_send()

    got_ref[...] = rbuf[...]


def combine_kernel(npos, got_ref, lp_ref, ent_ref):
    got = got_ref[...]
    values = pltpu.roll(got, LANES // 2, 2)
    top = jnp.max(got, axis=0)
    sums = jnp.sum(jnp.exp(got - top[None]) * values, axis=0)
    total = sums[:, :npos]
    weighted = pltpu.roll(sums, LANES - npos, 1)[:, :npos]
    pick = pltpu.roll(sums, LANES - 2 * npos, 1)[:, :npos]
    log_norm = top[:, :npos] + jnp.log(total)
    lp_ref[...] = pick - log_norm
    ent_ref[...] = log_norm - weighted / total


def solution(mesh):
    tp = mesh.shape["tp"]
    group = next(n for n in (SHARE, 2, 1) if mesh.shape["dp"] % n == 0)

    def local_part(hidden, norm_w, embedding, draft_ids):
        npos, depth = hidden.shape[1:]
        rows = embedding.shape[0] // group
        half = depth // HALVES
        nchunk = rows // CHUNK_ROWS
        any_spec = pl.BlockSpec(memory_space=pl.ANY)
        dma = pltpu.SemaphoreType.DMA
        got = pl.pallas_call(
            functools.partial(head_kernel, group, tp, rows),
            out_shape=jax.ShapeDtypeStruct((group * tp, 1, LANES), jnp.float32),
            in_specs=[any_spec] * 4,
            out_specs=pl.BlockSpec(memory_space=pltpu.VMEM),
            scratch_shapes=[
                pltpu.VMEM((npos, depth), jnp.bfloat16),
                pltpu.VMEM((depth,), jnp.bfloat16),
                pltpu.VMEM((1, npos), jnp.int32),
                pltpu.VMEM((group, HALVES, npos, half), jnp.float32),
                pltpu.VMEM((group, 1, LANES), jnp.int32),
                pltpu.VMEM((group * npos, depth), jnp.bfloat16),
                pltpu.VMEM((rows, depth), jnp.bfloat16),
                pltpu.VMEM((nchunk, CHUNK_ROWS, LANES), jnp.float32),
                pltpu.VMEM((group, 1, LANES), jnp.float32),
                pltpu.VMEM((group * tp, 1, LANES), jnp.float32),
                dma((3,)), dma((nchunk, HALVES)),
                dma((group,)), dma((group,)), dma((group,)), dma((group,)), dma((group,)), dma((group,)),
                dma, dma,
            ],
            compiler_params=pltpu.CompilerParams(
                collective_id=0, has_side_effects=True, vmem_limit_bytes=60 * 2**20),
        )(hidden, norm_w, embedding, draft_ids)
        return pl.pallas_call(
            functools.partial(combine_kernel, npos),
            out_shape=[jax.ShapeDtypeStruct((1, npos), jnp.float32)] * 2,
            in_specs=[pl.BlockSpec(memory_space=pltpu.VMEM)],
            out_specs=[pl.BlockSpec(memory_space=pltpu.VMEM)] * 2,
        )(got)

    return jax.shard_map(
        local_part, mesh=mesh,
        in_specs=(P("dp", None, None), P(None), P("tp", None), P("dp", None)),
        out_specs=(P("dp", None), P("dp", None)), check_vma=False)
```

```python
import functools

import jax
import jax.numpy as jnp
from jax import lax
from jax.experimental import pallas as pl
from jax.experimental.pallas import tpu as pltpu
from jax.sharding import PartitionSpec as P

EPS = 1e-6
MESH = pl.DeviceIdType.MESH
LANES = 128
HALVES = 2
PARTS = 2
SHARE = 4
OWN = (1024, 1024, 1024, 1024)
OWN_BEFORE = 3
CHUNK = 1024
BLOCKS = (1, 1, 1, 1, 1, 1, 1, 1)
FIRST_LOADS = 1
SECOND_LOADS = 5


def shared_chunks(rows):
    sizes = [CHUNK] * (rows // CHUNK)
    return sizes + ([rows % CHUNK] if rows % CHUNK else [])


def dot_rows(e, h):
    n = e.shape[0] // PARTS
    return [
        lax.dot_general(e[m * n:(m + 1) * n, :], h[...], (((1,), (1,)), ((), ())), preferred_element_type=jnp.float32)
        for m in range(PARTS)
    ]


def fold(z, first, want, state):
    n, width = z.shape
    z = z.reshape(n // 8, 8, width)
    row = lax.broadcasted_iota(jnp.int32, z.shape, 0) * 8 + first
    pick = jnp.sum(jnp.where(row == want[None], z, 0.0), axis=0)
    top = jnp.max(z, axis=0)
    if state is not None:
        top = jnp.maximum(top, state[0])
    e = jnp.exp(z - top[None])
    total = jnp.sum(e, axis=0)
    weighted = jnp.sum(e * z, axis=0)
    if state is not None:
        fade = jnp.exp(state[0] - top)
        total, weighted, pick = total + state[1] * fade, weighted + state[2] * fade, pick + state[3]
    return top, total, weighted, pick


def head_kernel(
    group, tp, hid_hbm, w_hbm, emb_hbm, ids_hbm, got_ref,
    hid_v, w_v, ids_v, hx, ids_x, h_own, h_all, ebuf, zo, zs, sbuf, rbuf,
    in_sem, esem, h_send, h_recv, f_send, f_recv, id_send, id_recv, s_send, s_recv,
):
    npos, depth = hid_v.shape
    half = depth // HALVES
    shard = emb_hbm.shape[0]
    n_own = sum(OWN)
    rows = (shard - n_own) // group
    shared = shared_chunks(rows)
    nsrc = group * tp
    width = group * npos

    dp_me = lax.axis_index("dp")
    tp_me = lax.axis_index("tp")
    q = lax.rem(dp_me, group)
    base = dp_me - q
    c = lax.rem(tp_me, 2)
    sibling = tp_me + 1 - 2 * c
    me = q * tp + tp_me

    def member(r):
        if group == 4:
            a, b = q // 2, lax.rem(q, 2)
            return lax.rem(a + r // 2, 2) * 2 + lax.rem(b + r % 2, 2)
        return lax.rem(q + r, group)

    others = tuple(range(group - 1, 0, -1))

    small = [
        pltpu.make_async_copy(hid_hbm.at[0], hid_v, in_sem.at[0]),
        pltpu.make_async_copy(w_hbm, w_v, in_sem.at[1]),
        pltpu.make_async_copy(ids_hbm, ids_v, in_sem.at[2]),
    ]
    for copy in small:
        copy.start()
    loads, spans, at = [], [], 0
    for j, n in enumerate(OWN + tuple(shared)):
        src = at if j < len(OWN) else at + q * rows
        loads.append(pltpu.make_async_copy(
            emb_hbm.at[pl.ds(src, n)], ebuf.at[pl.ds(at, n)], esem.at[j]))
        spans.append((at, n))
        at += n

    for copy in loads[:FIRST_LOADS]:
        copy.start()

    barrier = pltpu.get_barrier_semaphore()
    far_first = (tp // 2, tp // 2 + 1) + tuple(t for t in range(tp) if t not in (tp // 2, tp // 2 + 1))
    for r in others + (0,):
        for t in far_first:
            if r or t:
                pl.semaphore_signal(
                    barrier, inc=1, device_id=(base + member(r), lax.rem(tp_me + t, tp)), device_id_type=MESH)

    small[0].wait()
    small[1].wait()
    x = hid_v[...].astype(jnp.float32)
    scale = lax.rsqrt(jnp.mean(x * x, axis=-1, keepdims=True) + EPS)
    h = (x * scale * (1.0 + w_v[...].astype(jnp.float32).reshape(1, depth))).astype(jnp.bfloat16)
    h32 = h.astype(jnp.float32)
    for s in range(HALVES):
        hx[q, s] = h32[:, s * half:(s + 1) * half]
    h_own[...] = h
    small[2].wait()
    ids_x[q] = jnp.concatenate([ids_v[...], jnp.full((1, LANES - npos), -1, jnp.int32)], axis=1)

    pl.semaphore_wait(barrier, nsrc - 1)

    direct, ident, forward = {}, {}, {}
    for r in others:
        direct[r] = pltpu.make_async_remote_copy(
            src_ref=hx.at[q, c], dst_ref=hx.at[q, c], send_sem=h_send.at[r], recv_sem=h_recv.at[r],
            device_id=(base + member(r), tp_me), device_id_type=MESH)
        direct[r].start()
    for r in others:
        ident[r] = pltpu.make_async_remote_copy(
            src_ref=ids_x.at[q], dst_ref=ids_x.at[q], send_sem=id_send.at[r], recv_sem=id_recv.at[r],
            device_id=(base + member(r), tp_me), device_id_type=MESH)
        ident[r].start()
    for copy in loads[FIRST_LOADS:SECOND_LOADS]:
        copy.start()

    def place(p, s):
        h_all[s, pl.ds(pl.multiple_of(p * npos, npos), npos), :] = hx[p, s].astype(jnp.bfloat16)

    sub = lax.broadcasted_iota(jnp.int32, (8, npos), 0)
    want_own = jnp.broadcast_to(ids_x[q][:, :npos], (8, npos)) - tp_me * shard - sub
    own = None

    def own_fold(j, own):
        lo, n = spans[j]
        return fold(zo[j, :n, :], lo, want_own, own)

    def own_chunk(j, own):
        lo, n = spans[j]
        loads[j].wait()
        for m, part in enumerate(dot_rows(ebuf.at[pl.ds(lo, n)], h_own)):
            zo[j, m * (n // PARTS):(m + 1) * (n // PARTS), :] = part
        return own_fold(j - 1, own) if j else own

    for j in range(OWN_BEFORE):
        own = own_chunk(j, own)

    for r in others:
        p = member(r)
        direct[r].wait_recv()
        forward[r] = pltpu.make_async_remote_copy(
            src_ref=hx.at[p, c], dst_ref=hx.at[p, c], send_sem=f_send.at[r], recv_sem=f_recv.at[r],
            device_id=(dp_me, sibling), device_id_type=MESH)
        forward[r].start()
    for copy in loads[SECOND_LOADS:]:
        copy.start()
    for r in others:
        ident[r].wait_recv()
        place(member(r), c)
    for s in range(HALVES):
        place(q, s)

    lane = lax.broadcasted_iota(jnp.int32, (8, LANES), 1)
    want = jnp.full((8, LANES), -1, jnp.int32)
    for p in range(group):
        moved = jnp.broadcast_to(ids_x[p], (8, LANES))
        if p:
            moved = pltpu.roll(moved, p * npos, 1)
        want = jnp.where((lane >= p * npos) & (lane < (p + 1) * npos), moved, want)
    first_row = tp_me * shard + n_own + q * rows
    want = (want - first_row - lax.broadcasted_iota(jnp.int32, (8, LANES), 0))[:, :width]

    for j in range(OWN_BEFORE, len(OWN)):
        own = own_chunk(j, own)
    own = own_fold(len(OWN) - 1, own)

    mine = (lane >= q * npos) & (lane < (q + 1) * npos)

    def spread(v, other):
        v = jnp.concatenate([v, jnp.zeros((8, LANES - npos), jnp.float32)], axis=1)
        return jnp.where(mine, pltpu.roll(v, q * npos, 1), other)[:, :width]

    state = tuple(spread(v, other) for v, other in zip(own, (-jnp.inf, 0.0, 0.0, 0.0)))

    for r in others:
        forward[r].wait_recv()
        place(member(r), 1 - c)

    h_pos = jnp.concatenate([h_all[s] for s in range(HALVES)], axis=1)
    n_chunks = len(shared)
    at = 0
    for size in BLOCKS:
        end = min(at + size, n_chunks)
        for j in range(at, end):
            loads[len(OWN) + j].wait()
        for j in range(at, end):
            lo, n = spans[len(OWN) + j]
            for m, part in enumerate(dot_rows(ebuf.at[pl.ds(lo, n)], h_pos)):
                zs[j, m * (n // PARTS):(m + 1) * (n // PARTS), :] = part
            if j:
                before, count = spans[len(OWN) + j - 1]
                state = fold(zs[j - 1, :count, :], before - n_own, want, state)
        at = end
    lo, n = spans[-1]
    state = fold(zs[n_chunks - 1, :n, :], lo - n_own, want, state)

    top8, total8, weighted8, pick8 = (
        jnp.concatenate([v, jnp.zeros((8, LANES - width), jnp.float32)], axis=1) for v in state)
    top = jnp.max(top8, axis=0, keepdims=True)
    fade = jnp.exp(top8 - top)
    full = lambda v: jnp.broadcast_to(v, (8, LANES))
    top = full(top)
    total = full(jnp.sum(total8 * fade, axis=0, keepdims=True))
    weighted = full(jnp.sum(weighted8 * fade, axis=0, keepdims=True))
    pick = full(jnp.sum(pick8, axis=0, keepdims=True))
    for p in range(group):
        message = jnp.zeros((8, LANES), jnp.float32)
        for at, v in ((0, top), (1, top), (4, total), (5, weighted), (6, pick)):
            shift = (at * npos - p * npos) % LANES
            moved = pltpu.roll(v, shift, 1) if shift else v
            message = jnp.where((lane >= at * npos) & (lane < (at + 1) * npos), moved, message)
        sbuf[p] = message[:1]

    for r in others + (0,):
        for t in far_first:
            if r or t:
                pltpu.make_async_remote_copy(
                    src_ref=sbuf.at[member(r)], dst_ref=rbuf.at[me], send_sem=s_send, recv_sem=s_recv,
                    device_id=(base + member(r), lax.rem(tp_me + t, tp)), device_id_type=MESH).start()
    rbuf[me] = sbuf[q]
    for copies in (direct, ident, forward):
        for copy in copies.values():
            copy.wait_send()
    everyone = pltpu.make_async_remote_copy(
        src_ref=rbuf.at[pl.ds(0, nsrc - 1)], dst_ref=rbuf.at[pl.ds(0, nsrc - 1)], send_sem=s_send, recv_sem=s_recv,
        device_id=(dp_me, tp_me), device_id_type=MESH)
    everyone.wait_recv()
    everyone.wait_send()
    got_ref[...] = rbuf[...]


def combine_kernel(npos, got_ref, lp_ref, ent_ref):
    got = got_ref[...]
    values = pltpu.roll(got, LANES // 2, 2)
    top = jnp.max(got, axis=0)
    sums = jnp.sum(jnp.exp(got - top[None]) * values, axis=0)
    total = sums[:, :npos]
    weighted = pltpu.roll(sums, LANES - npos, 1)[:, :npos]
    pick = pltpu.roll(sums, LANES - 2 * npos, 1)[:, :npos]
    log_norm = top[:, :npos] + jnp.log(total)
    lp_ref[...] = pick - log_norm
    ent_ref[...] = log_norm - weighted / total


def solution(mesh):
    tp = mesh.shape["tp"]
    group = next(n for n in (SHARE, 2, 1) if mesh.shape["dp"] % n == 0)

    def local_part(hidden, norm_w, embedding, draft_ids):
        npos, depth = hidden.shape[1:]
        shard = embedding.shape[0]
        rows = (shard - sum(OWN)) // group
        half = depth // HALVES
        n_shared = len(shared_chunks(rows))
        any_spec = pl.BlockSpec(memory_space=pl.ANY)
        dma = pltpu.SemaphoreType.DMA
        got = pl.pallas_call(
            functools.partial(head_kernel, group, tp),
            out_shape=pltpu.VMEM((group * tp, 1, LANES), jnp.float32),
            in_specs=[any_spec] * 4,
            out_specs=pl.BlockSpec(memory_space=pltpu.VMEM),
            scratch_shapes=[
                pltpu.VMEM((npos, depth), jnp.bfloat16),
                pltpu.VMEM((depth,), jnp.bfloat16),
                pltpu.VMEM((1, npos), jnp.int32),
                pltpu.VMEM((group, HALVES, npos, half), jnp.float32),
                pltpu.VMEM((group, 1, LANES), jnp.int32),
                pltpu.VMEM((npos, depth), jnp.bfloat16),
                pltpu.VMEM((HALVES, group * npos, half), jnp.bfloat16),
                pltpu.VMEM((sum(OWN) + rows, depth), jnp.bfloat16),
                pltpu.VMEM((len(OWN), max(OWN), npos), jnp.float32),
                pltpu.VMEM((n_shared, CHUNK, group * npos), jnp.float32),
                pltpu.VMEM((group, 1, LANES), jnp.float32),
                pltpu.VMEM((group * tp, 1, LANES), jnp.float32),
                dma((3,)), dma((len(OWN) + n_shared,)),
                dma((group,)), dma((group,)), dma((group,)), dma((group,)), dma((group,)), dma((group,)),
                dma, dma,
            ],
            compiler_params=pltpu.CompilerParams(
                collective_id=0, has_side_effects=True, vmem_limit_bytes=60 * 2**20),
        )(hidden, norm_w, embedding, draft_ids)
        return pl.pallas_call(
            functools.partial(combine_kernel, npos),
            out_shape=[jax.ShapeDtypeStruct((1, npos), jnp.float32)] * 2,
            in_specs=[pl.BlockSpec(memory_space=pltpu.VMEM)],
            out_specs=[pl.BlockSpec(memory_space=pltpu.VMEM)] * 2,
            compiler_params=pltpu.CompilerParams(vmem_limit_bytes=2**20),
        )(got)

    return jax.shard_map(
        local_part, mesh=mesh,
        in_specs=(P("dp", None, None), P(None), P("tp", None), P("dp", None)),
        out_specs=(P("dp", None), P("dp", None)), check_vma=False)
```

```python
import functools

import jax
import jax.numpy as jnp
from jax import lax
from jax.experimental import pallas as pl
from jax.experimental.pallas import tpu as pltpu
from jax.sharding import PartitionSpec as P

EPS = 1e-6
MESH = pl.DeviceIdType.MESH
LANES = 128
HALVES = 2
PARTS = 2
SHARE = 4
OWN = (1024, 1024, 1024, 1024)
OWN_BEFORE = 3
CHUNK = 1024
BLOCKS = (1, 2, 2, 2)
FIRST_LOADS = 1
SECOND_LOADS = 5


def shared_chunks(rows):
    sizes = [CHUNK] * (rows // CHUNK)
    return sizes + ([rows % CHUNK] if rows % CHUNK else [])


def dot_rows(e, h):
    n = e.shape[0] // PARTS
    return [
        lax.dot_general(e[m * n:(m + 1) * n, :], h[...], (((1,), (1,)), ((), ())), preferred_element_type=jnp.float32)
        for m in range(PARTS)
    ]


def fold(z, first, want, state):
    n, width = z.shape
    z = z.reshape(n // 8, 8, width)
    row = lax.broadcasted_iota(jnp.int32, z.shape, 0) * 8 + first
    pick = jnp.sum(jnp.where(row == want[None], z, 0.0), axis=0)
    top = jnp.max(z, axis=0)
    if state is not None:
        top = jnp.maximum(top, state[0])
    e = jnp.exp(z - top[None])
    total = jnp.sum(e, axis=0)
    weighted = jnp.sum(e * z, axis=0)
    if state is not None:
        fade = jnp.exp(state[0] - top)
        total, weighted, pick = total + state[1] * fade, weighted + state[2] * fade, pick + state[3]
    return top, total, weighted, pick


def head_kernel(
    group, tp, hid_hbm, w_hbm, emb_hbm, ids_hbm, got_ref,
    hid_v, w_v, ids_v, hx, ids_x, h_own, h_all, ebuf, zo, zs, sbuf, rbuf,
    in_sem, esem, h_send, h_recv, f_send, f_recv, id_send, id_recv, s_send, s_recv, token,
):
    npos, depth = hid_v.shape
    half = depth // HALVES
    shard = emb_hbm.shape[0]
    n_own = sum(OWN)
    rows = (shard - n_own) // group
    shared = shared_chunks(rows)
    nsrc = group * tp
    width = group * npos

    dp_me = lax.axis_index("dp")
    tp_me = lax.axis_index("tp")
    q = lax.rem(dp_me, group)
    base = dp_me - q
    c = lax.rem(tp_me, 2)
    sibling = tp_me + 1 - 2 * c
    me = q * tp + tp_me

    def member(r):
        if group == 4:
            a, b = q // 2, lax.rem(q, 2)
            return lax.rem(a + r // 2, 2) * 2 + lax.rem(b + r % 2, 2)
        return lax.rem(q + r, group)

    others = tuple(range(group - 1, 0, -1))

    small = [
        pltpu.make_async_copy(hid_hbm.at[0], hid_v, in_sem.at[0]),
        pltpu.make_async_copy(w_hbm, w_v, in_sem.at[1]),
        pltpu.make_async_copy(ids_hbm, ids_v, in_sem.at[2]),
    ]
    for copy in small:
        copy.start()
    loads, spans, at = [], [], 0
    for j, n in enumerate(OWN + tuple(shared)):
        src = at if j < len(OWN) else at + q * rows
        loads.append(pltpu.make_async_copy(
            emb_hbm.at[pl.ds(src, n)], ebuf.at[pl.ds(at, n)], esem.at[j]))
        spans.append((at, n))
        at += n

    for copy in loads[:FIRST_LOADS]:
        copy.start()

    barrier = pltpu.get_barrier_semaphore()
    beside = (lax.rem(tp_me + 2, tp), lax.rem(tp_me + tp - 2, tp))
    near = [(base + member(r), tp_me) for r in others] + [(dp_me, sibling)] + [(dp_me, t) for t in beside]
    for device in near:
        pl.semaphore_signal(barrier, inc=1, device_id=device, device_id_type=MESH)

    small[0].wait()
    small[1].wait()
    x = hid_v[...].astype(jnp.float32)
    scale = lax.rsqrt(jnp.mean(x * x, axis=-1, keepdims=True) + EPS)
    h = (x * scale * (1.0 + w_v[...].astype(jnp.float32).reshape(1, depth))).astype(jnp.bfloat16)
    h32 = h.astype(jnp.float32)
    for s in range(HALVES):
        hx[q, s] = h32[:, s * half:(s + 1) * half]
    h_own[...] = h
    small[2].wait()
    ids_x[q] = jnp.concatenate([ids_v[...], jnp.full((1, LANES - npos), -1, jnp.int32)], axis=1)

    pl.semaphore_wait(barrier, len(near))

    direct, ident, forward = {}, {}, {}
    for r in others:
        direct[r] = pltpu.make_async_remote_copy(
            src_ref=hx.at[q, c], dst_ref=hx.at[q, c], send_sem=h_send.at[r], recv_sem=h_recv.at[r],
            device_id=(base + member(r), tp_me), device_id_type=MESH)
        direct[r].start()
    for r in others:
        ident[r] = pltpu.make_async_remote_copy(
            src_ref=ids_x.at[q], dst_ref=ids_x.at[q], send_sem=id_send.at[r], recv_sem=id_recv.at[r],
            device_id=(base + member(r), tp_me), device_id_type=MESH)
        ident[r].start()
    for copy in loads[FIRST_LOADS:SECOND_LOADS]:
        copy.start()

    def tell(k):
        for device in near[-2:] if k < 2 else near[-3:-2]:
            pl.semaphore_signal(token.at[k], inc=1, device_id=device, device_id_type=MESH)

    def hear(k):
        pl.semaphore_wait(token.at[k], 2 if k < 2 else 1)

    tell(0)

    def place(p, s):
        h_all[s, pl.ds(pl.multiple_of(p * npos, npos), npos), :] = hx[p, s].astype(jnp.bfloat16)

    sub = lax.broadcasted_iota(jnp.int32, (8, npos), 0)
    want_own = jnp.broadcast_to(ids_x[q][:, :npos], (8, npos)) - tp_me * shard - sub
    own = None

    def own_fold(j, own):
        lo, n = spans[j]
        return fold(zo[j, :n, :], lo, want_own, own)

    def own_chunk(j, own):
        lo, n = spans[j]
        loads[j].wait()
        for m, part in enumerate(dot_rows(ebuf.at[pl.ds(lo, n)], h_own)):
            zo[j, m * (n // PARTS):(m + 1) * (n // PARTS), :] = part
        return own_fold(j - 1, own) if j else own

    for j in range(OWN_BEFORE):
        own = own_chunk(j, own)
        if j == 1:
            hear(0)
            tell(1)

    for r in others:
        p = member(r)
        direct[r].wait_recv()
        forward[r] = pltpu.make_async_remote_copy(
            src_ref=hx.at[p, c], dst_ref=hx.at[p, c], send_sem=f_send.at[r], recv_sem=f_recv.at[r],
            device_id=(dp_me, sibling), device_id_type=MESH)
        forward[r].start()
    for copy in loads[SECOND_LOADS:]:
        copy.start()
    hear(1)
    tell(2)
    for r in others:
        ident[r].wait_recv()
        place(member(r), c)
    for s in range(HALVES):
        place(q, s)

    lane = lax.broadcasted_iota(jnp.int32, (8, LANES), 1)
    want = jnp.full((8, LANES), -1, jnp.int32)
    for p in range(group):
        moved = jnp.broadcast_to(ids_x[p], (8, LANES))
        if p:
            moved = pltpu.roll(moved, p * npos, 1)
        want = jnp.where((lane >= p * npos) & (lane < (p + 1) * npos), moved, want)
    first_row = tp_me * shard + n_own + q * rows
    want = (want - first_row - lax.broadcasted_iota(jnp.int32, (8, LANES), 0))[:, :width]

    for j in range(OWN_BEFORE, len(OWN)):
        own = own_chunk(j, own)
    own = own_fold(len(OWN) - 1, own)

    mine = (lane >= q * npos) & (lane < (q + 1) * npos)

    def spread(v, other):
        v = jnp.concatenate([v, jnp.zeros((8, LANES - npos), jnp.float32)], axis=1)
        return jnp.where(mine, pltpu.roll(v, q * npos, 1), other)[:, :width]

    state = tuple(spread(v, other) for v, other in zip(own, (-jnp.inf, 0.0, 0.0, 0.0)))

    for r in others:
        forward[r].wait_recv()
        place(member(r), 1 - c)

    hear(2)

    h_pos = jnp.concatenate([h_all[s] for s in range(HALVES)], axis=1)
    n_chunks = len(shared)
    at = 0
    for size in BLOCKS:
        end = min(at + size, n_chunks)
        for j in range(at, end):
            loads[len(OWN) + j].wait()
        for j in range(at, end):
            lo, n = spans[len(OWN) + j]
            for m, part in enumerate(dot_rows(ebuf.at[pl.ds(lo, n)], h_pos)):
                zs[j, m * (n // PARTS):(m + 1) * (n // PARTS), :] = part
            if j:
                before, count = spans[len(OWN) + j - 1]
                state = fold(zs[j - 1, :count, :], before - n_own, want, state)
        at = end
    lo, n = spans[-1]
    state = fold(zs[n_chunks - 1, :n, :], lo - n_own, want, state)

    top8, total8, weighted8, pick8 = (
        jnp.concatenate([v, jnp.zeros((8, LANES - width), jnp.float32)], axis=1) for v in state)
    top = jnp.max(top8, axis=0, keepdims=True)
    fade = jnp.exp(top8 - top)
    full = lambda v: jnp.broadcast_to(v, (8, LANES))
    top = full(top)
    total = full(jnp.sum(total8 * fade, axis=0, keepdims=True))
    weighted = full(jnp.sum(weighted8 * fade, axis=0, keepdims=True))
    pick = full(jnp.sum(pick8, axis=0, keepdims=True))
    for p in range(group):
        message = jnp.zeros((8, LANES), jnp.float32)
        for at, v in ((0, top), (1, top), (4, total), (5, weighted), (6, pick)):
            shift = (at * npos - p * npos) % LANES
            moved = pltpu.roll(v, shift, 1) if shift else v
            message = jnp.where((lane >= at * npos) & (lane < (at + 1) * npos), moved, message)
        sbuf[p] = message[:1]

    far_first = (tp // 2, tp // 2 + 1) + tuple(t for t in range(tp) if t not in (tp // 2, tp // 2 + 1))
    for r in others + (0,):
        for t in far_first:
            if r or t:
                pltpu.make_async_remote_copy(
                    src_ref=sbuf.at[member(r)], dst_ref=rbuf.at[me], send_sem=s_send, recv_sem=s_recv,
                    device_id=(base + member(r), lax.rem(tp_me + t, tp)), device_id_type=MESH).start()
    rbuf[me] = sbuf[q]
    for copies in (direct, ident, forward):
        for copy in copies.values():
            copy.wait_send()
    everyone = pltpu.make_async_remote_copy(
        src_ref=rbuf.at[pl.ds(0, nsrc - 1)], dst_ref=rbuf.at[pl.ds(0, nsrc - 1)], send_sem=s_send, recv_sem=s_recv,
        device_id=(dp_me, tp_me), device_id_type=MESH)
    everyone.wait_recv()
    everyone.wait_send()
    got_ref[...] = rbuf[...]


def combine_kernel(npos, got_ref, lp_ref, ent_ref):
    got = got_ref[...]
    values = pltpu.roll(got, LANES // 2, 2)
    top = jnp.max(got, axis=0)
    sums = jnp.sum(jnp.exp(got - top[None]) * values, axis=0)
    total = sums[:, :npos]
    weighted = pltpu.roll(sums, LANES - npos, 1)[:, :npos]
    pick = pltpu.roll(sums, LANES - 2 * npos, 1)[:, :npos]
    log_norm = top[:, :npos] + jnp.log(total)
    lp_ref[...] = pick - log_norm
    ent_ref[...] = log_norm - weighted / total


def solution(mesh):
    tp = mesh.shape["tp"]
    group = next(n for n in (SHARE, 2, 1) if mesh.shape["dp"] % n == 0)

    def local_part(hidden, norm_w, embedding, draft_ids):
        npos, depth = hidden.shape[1:]
        shard = embedding.shape[0]
        rows = (shard - sum(OWN)) // group
        half = depth // HALVES
        n_shared = len(shared_chunks(rows))
        any_spec = pl.BlockSpec(memory_space=pl.ANY)
        dma = pltpu.SemaphoreType.DMA
        got = pl.pallas_call(
            functools.partial(head_kernel, group, tp),
            out_shape=pltpu.VMEM((group * tp, 1, LANES), jnp.float32),
            in_specs=[any_spec] * 4,
            out_specs=pl.BlockSpec(memory_space=pltpu.VMEM),
            scratch_shapes=[
                pltpu.VMEM((npos, depth), jnp.bfloat16),
                pltpu.VMEM((depth,), jnp.bfloat16),
                pltpu.VMEM((1, npos), jnp.int32),
                pltpu.VMEM((group, HALVES, npos, half), jnp.float32),
                pltpu.VMEM((group, 1, LANES), jnp.int32),
                pltpu.VMEM((npos, depth), jnp.bfloat16),
                pltpu.VMEM((HALVES, group * npos, half), jnp.bfloat16),
                pltpu.VMEM((sum(OWN) + rows, depth), jnp.bfloat16),
                pltpu.VMEM((len(OWN), max(OWN), npos), jnp.float32),
                pltpu.VMEM((n_shared, CHUNK, group * npos), jnp.float32),
                pltpu.VMEM((group, 1, LANES), jnp.float32),
                pltpu.VMEM((group * tp, 1, LANES), jnp.float32),
                dma((3,)), dma((len(OWN) + n_shared,)),
                dma((group,)), dma((group,)), dma((group,)), dma((group,)), dma((group,)), dma((group,)),
                dma, dma, pltpu.SemaphoreType.REGULAR((3,)),
            ],
            compiler_params=pltpu.CompilerParams(
                collective_id=0, has_side_effects=True, vmem_limit_bytes=60 * 2**20),
        )(hidden, norm_w, embedding, draft_ids)
        return pl.pallas_call(
            functools.partial(combine_kernel, npos),
            out_shape=[jax.ShapeDtypeStruct((1, npos), jnp.float32)] * 2,
            in_specs=[pl.BlockSpec(memory_space=pltpu.VMEM)],
            out_specs=[pl.BlockSpec(memory_space=pltpu.VMEM)] * 2,
            compiler_params=pltpu.CompilerParams(vmem_limit_bytes=2**20),
        )(got)

    return jax.shard_map(
        local_part, mesh=mesh,
        in_specs=(P("dp", None, None), P(None), P("tp", None), P("dp", None)),
        out_specs=(P("dp", None), P("dp", None)), check_vma=False)
```

```python
import functools

import jax
import jax.numpy as jnp
from jax import lax
from jax.experimental import pallas as pl
from jax.experimental.pallas import tpu as pltpu
from jax.sharding import PartitionSpec as P

EPS = 1e-6
MESH = pl.DeviceIdType.MESH
LANES = 128
HALVES = 2
PARTS = 2
SHARE = 4
OWN = (1280, 1280)
CHUNK = 1024
UNIT = 512
EARLY = 2
BLOCKS = (1, 1, 1, 1, 2)
FIRST_LOADS = 1
SECOND_LOADS = 4


def shared_chunks(rows):
    sizes = [CHUNK] * (rows // CHUNK)
    return sizes + ([rows % CHUNK] if rows % CHUNK else [])


def dot_rows(e, h):
    n = e.shape[0] // PARTS
    return [
        lax.dot_general(e[m * n:(m + 1) * n, :], h, (((1,), (1,)), ((), ())), preferred_element_type=jnp.float32)
        for m in range(PARTS)
    ]


def fold(z, first, want, state):
    n, width = z.shape
    z = z.reshape(n // 8, 8, width)
    row = lax.broadcasted_iota(jnp.int32, z.shape, 0) * 8 + first
    pick = jnp.sum(jnp.where(row == want[None], z, 0.0), axis=0)
    top = jnp.max(z, axis=0)
    if state is not None:
        top = jnp.maximum(top, state[0])
    e = jnp.exp(z - top[None])
    total = jnp.sum(e, axis=0)
    weighted = jnp.sum(e * z, axis=0)
    if state is not None:
        fade = jnp.exp(state[0] - top)
        total, weighted, pick = total + state[1] * fade, weighted + state[2] * fade, pick + state[3]
    return top, total, weighted, pick


def head_kernel(
    group, tp, hid_hbm, w_hbm, emb_hbm, ids_hbm, got_ref,
    hid_v, w_v, ids_v, hx, ids_x, h_own, h_all, ebuf, zo, zs, sbuf, rbuf,
    in_sem, esem, h_send, h_recv, f_send, f_recv, id_send, id_recv, s_send, s_recv, token,
):
    npos, depth = hid_v.shape
    half = depth // HALVES
    shard = emb_hbm.shape[0]
    n_own = sum(OWN)
    rows = (shard - n_own) // group
    shared = shared_chunks(rows)
    nsrc = group * tp
    width = group * npos

    dp_me = lax.axis_index("dp")
    tp_me = lax.axis_index("tp")
    q = lax.rem(dp_me, group)
    base = dp_me - q
    c = lax.rem(tp_me, 2)
    sibling = tp_me + 1 - 2 * c
    me = q * tp + tp_me

    def member(r):
        if group == 4:
            a, b = q // 2, lax.rem(q, 2)
            return lax.rem(a + r // 2, 2) * 2 + lax.rem(b + r % 2, 2)
        return lax.rem(q + r, group)

    others = tuple(range(group - 1, 0, -1))

    small = [
        pltpu.make_async_copy(hid_hbm.at[0], hid_v, in_sem.at[0]),
        pltpu.make_async_copy(w_hbm, w_v, in_sem.at[1]),
        pltpu.make_async_copy(ids_hbm, ids_v, in_sem.at[2]),
    ]
    for copy in small:
        copy.start()
    loads, spans, at = [], [], 0
    for j, n in enumerate(OWN + tuple(shared)):
        src = at if j < len(OWN) else at + q * rows
        loads.append(pltpu.make_async_copy(
            emb_hbm.at[pl.ds(src, n)], ebuf.at[pl.ds(at, n)], esem.at[j]))
        spans.append((at, n))
        at += n

    for copy in loads[:FIRST_LOADS]:
        copy.start()

    barrier = pltpu.get_barrier_semaphore()
    beside = (lax.rem(tp_me + 2, tp), lax.rem(tp_me + tp - 2, tp))
    near = [(base + member(r), tp_me) for r in others] + [(dp_me, sibling)] + [(dp_me, t) for t in beside]
    for device in near:
        pl.semaphore_signal(barrier, inc=1, device_id=device, device_id_type=MESH)

    small[0].wait()
    small[1].wait()
    x = hid_v[...].astype(jnp.float32)
    scale = lax.rsqrt(jnp.mean(x * x, axis=-1, keepdims=True) + EPS)
    h = (x * scale * (1.0 + w_v[...].astype(jnp.float32).reshape(1, depth))).astype(jnp.bfloat16)
    h32 = h.astype(jnp.float32)
    for s in range(HALVES):
        hx[q, s] = h32[:, s * half:(s + 1) * half]
    h_own[...] = h
    small[2].wait()
    ids_x[q] = jnp.concatenate([ids_v[...], jnp.full((1, LANES - npos), -1, jnp.int32)], axis=1)

    pl.semaphore_wait(barrier, len(near))

    direct, ident, forward = {}, {}, {}
    for r in others:
        direct[r] = pltpu.make_async_remote_copy(
            src_ref=hx.at[q, c], dst_ref=hx.at[q, c], send_sem=h_send.at[r], recv_sem=h_recv.at[r],
            device_id=(base + member(r), tp_me), device_id_type=MESH)
        direct[r].start()
    for r in others:
        ident[r] = pltpu.make_async_remote_copy(
            src_ref=ids_x.at[q], dst_ref=ids_x.at[q], send_sem=id_send.at[r], recv_sem=id_recv.at[r],
            device_id=(base + member(r), tp_me), device_id_type=MESH)
        ident[r].start()
    for copy in loads[FIRST_LOADS:SECOND_LOADS]:
        copy.start()

    def tell(k):
        for device in near[-2:] if k < 2 else near[-3:-2]:
            pl.semaphore_signal(token.at[k], inc=1, device_id=device, device_id_type=MESH)

    def hear(k):
        pl.semaphore_wait(token.at[k], 2 if k < 2 else 1)

    tell(0)

    def place(p, s):
        h_all[s, pl.ds(pl.multiple_of(p * npos, npos), npos), :] = hx[p, s].astype(jnp.bfloat16)

    sub = lax.broadcasted_iota(jnp.int32, (8, npos), 0)
    want_own = jnp.broadcast_to(ids_x[q][:, :npos], (8, npos)) - tp_me * shard - sub
    own = None

    def own_fold(j, own):
        lo, n = spans[j]
        return fold(zo[j, :n, :], lo, want_own, own)

    h_mine = h_own[...]
    for j in range(len(OWN)):
        lo, n = spans[j]
        loads[j].wait()
        for m, part in enumerate(dot_rows(ebuf.at[pl.ds(lo, n)], h_mine)):
            zo[j, m * (n // PARTS):(m + 1) * (n // PARTS), :] = part
        if j:
            own = own_fold(j - 1, own)
        if j == 0:
            hear(0)
            tell(1)
    for r in others:
        p = member(r)
        direct[r].wait_recv()
        forward[r] = pltpu.make_async_remote_copy(
            src_ref=hx.at[p, c], dst_ref=hx.at[p, c], send_sem=f_send.at[r], recv_sem=f_recv.at[r],
            device_id=(dp_me, sibling), device_id_type=MESH)
        forward[r].start()
    for copy in loads[SECOND_LOADS:]:
        copy.start()
    hear(1)
    tell(2)
    for r in others:
        ident[r].wait_recv()
        place(member(r), c)
    for s in range(HALVES):
        place(q, s)

    lane = lax.broadcasted_iota(jnp.int32, (8, LANES), 1)
    want = jnp.full((8, LANES), -1, jnp.int32)
    for p in range(group):
        moved = jnp.broadcast_to(ids_x[p], (8, LANES))
        if p:
            moved = pltpu.roll(moved, p * npos, 1)
        want = jnp.where((lane >= p * npos) & (lane < (p + 1) * npos), moved, want)
    first_row = tp_me * shard + n_own + q * rows
    want = (want - first_row - lax.broadcasted_iota(jnp.int32, (8, LANES), 0))[:, :width]

    units = []
    for j in range(len(shared)):
        lo, n = spans[len(OWN) + j]
        units.append([(lo + u, min(UNIT, n - u)) for u in range(0, n, UNIT)])
    order = [unit for chunk in units for unit in chunk]

    def keep(unit, col, width_in, h, add):
        lo, n = unit
        for m, part in enumerate(dot_rows(ebuf.at[pl.ds(lo, n), pl.ds(col, width_in)], h)):
            at = slice(m * (n // PARTS), (m + 1) * (n // PARTS))
            u = order.index(unit)
            zs[u, at, :] = part + zs[u, at, :] if add else part

    def shared_fold(unit, state):
        lo, n = unit
        return fold(zs[order.index(unit), :n, :], lo - n_own, want, state)

    for j in range(EARLY):
        loads[len(OWN) + j].wait()
        for unit in units[j]:
            keep(unit, pl.multiple_of(c * half, half), half, h_all[c], False)
        if j == 0:
            own = own_fold(len(OWN) - 1, own)

    mine = (lane >= q * npos) & (lane < (q + 1) * npos)

    def spread(v, other):
        v = jnp.concatenate([v, jnp.zeros((8, LANES - npos), jnp.float32)], axis=1)
        return jnp.where(mine, pltpu.roll(v, q * npos, 1), other)[:, :width]

    state = tuple(spread(v, other) for v, other in zip(own, (-jnp.inf, 0.0, 0.0, 0.0)))

    for r in others:
        forward[r].wait_recv()
        place(member(r), 1 - c)
    hear(2)
    pending = None
    for j in range(EARLY):
        for unit in units[j]:
            keep(unit, pl.multiple_of((1 - c) * half, half), half, h_all[1 - c], True)
            if pending is not None:
                state = shared_fold(pending, state)
            pending = unit

    h_pos = jnp.concatenate([h_all[s] for s in range(HALVES)], axis=1)
    at = EARLY
    for size in BLOCKS:
        end = min(at + size, len(shared))
        for j in range(at, end):
            loads[len(OWN) + j].wait()
        for j in range(at, end):
            for unit in units[j]:
                keep(unit, 0, depth, h_pos, False)
                state = shared_fold(pending, state)
                pending = unit
        at = end
    state = shared_fold(pending, state)

    top8, total8, weighted8, pick8 = (
        jnp.concatenate([v, jnp.zeros((8, LANES - width), jnp.float32)], axis=1) for v in state)
    top = jnp.max(top8, axis=0, keepdims=True)
    fade = jnp.exp(top8 - top)
    full = lambda v: jnp.broadcast_to(v, (8, LANES))
    top = full(top)
    total = full(jnp.sum(total8 * fade, axis=0, keepdims=True))
    weighted = full(jnp.sum(weighted8 * fade, axis=0, keepdims=True))
    pick = full(jnp.sum(pick8, axis=0, keepdims=True))
    for p in range(group):
        message = jnp.zeros((8, LANES), jnp.float32)
        for at, v in ((0, top), (1, top), (4, total), (5, weighted), (6, pick)):
            shift = (at * npos - p * npos) % LANES
            moved = pltpu.roll(v, shift, 1) if shift else v
            message = jnp.where((lane >= at * npos) & (lane < (at + 1) * npos), moved, message)
        sbuf[p] = message[:1]

    far_first = (tp // 2, tp // 2 + 1) + tuple(t for t in range(tp) if t not in (tp // 2, tp // 2 + 1))
    for r in others + (0,):
        for t in far_first:
            if r or t:
                pltpu.make_async_remote_copy(
                    src_ref=sbuf.at[member(r)], dst_ref=rbuf.at[me], send_sem=s_send, recv_sem=s_recv,
                    device_id=(base + member(r), lax.rem(tp_me + t, tp)), device_id_type=MESH).start()
    rbuf[me] = sbuf[q]
    for copies in (direct, ident, forward):
        for copy in copies.values():
            copy.wait_send()
    everyone = pltpu.make_async_remote_copy(
        src_ref=rbuf.at[pl.ds(0, nsrc - 1)], dst_ref=rbuf.at[pl.ds(0, nsrc - 1)], send_sem=s_send, recv_sem=s_recv,
        device_id=(dp_me, tp_me), device_id_type=MESH)
    everyone.wait_recv()
    everyone.wait_send()
    got_ref[...] = rbuf[...]


def combine_kernel(npos, got_ref, lp_ref, ent_ref):
    got = got_ref[...]
    values = pltpu.roll(got, LANES // 2, 2)
    top = jnp.max(got, axis=0)
    sums = jnp.sum(jnp.exp(got - top[None]) * values, axis=0)
    total = sums[:, :npos]
    weighted = pltpu.roll(sums, LANES - npos, 1)[:, :npos]
    pick = pltpu.roll(sums, LANES - 2 * npos, 1)[:, :npos]
    log_norm = top[:, :npos] + jnp.log(total)
    lp_ref[...] = pick - log_norm
    ent_ref[...] = log_norm - weighted / total


def solution(mesh):
    tp = mesh.shape["tp"]
    group = next(n for n in (SHARE, 2, 1) if mesh.shape["dp"] % n == 0)

    def local_part(hidden, norm_w, embedding, draft_ids):
        npos, depth = hidden.shape[1:]
        shard = embedding.shape[0]
        rows = (shard - sum(OWN)) // group
        half = depth // HALVES
        n_shared = len(shared_chunks(rows))
        n_units = sum(-(-n // UNIT) for n in shared_chunks(rows))
        any_spec = pl.BlockSpec(memory_space=pl.ANY)
        dma = pltpu.SemaphoreType.DMA
        got = pl.pallas_call(
            functools.partial(head_kernel, group, tp),
            out_shape=pltpu.VMEM((group * tp, 1, LANES), jnp.float32),
            in_specs=[any_spec] * 4,
            out_specs=pl.BlockSpec(memory_space=pltpu.VMEM),
            scratch_shapes=[
                pltpu.VMEM((npos, depth), jnp.bfloat16),
                pltpu.VMEM((depth,), jnp.bfloat16),
                pltpu.VMEM((1, npos), jnp.int32),
                pltpu.VMEM((group, HALVES, npos, half), jnp.float32),
                pltpu.VMEM((group, 1, LANES), jnp.int32),
                pltpu.VMEM((npos, depth), jnp.bfloat16),
                pltpu.VMEM((HALVES, group * npos, half), jnp.bfloat16),
                pltpu.VMEM((sum(OWN) + rows, depth), jnp.bfloat16),
                pltpu.VMEM((len(OWN), max(OWN), npos), jnp.float32),
                pltpu.VMEM((n_units, UNIT, group * npos), jnp.float32),
                pltpu.VMEM((group, 1, LANES), jnp.float32),
                pltpu.VMEM((group * tp, 1, LANES), jnp.float32),
                dma((3,)), dma((len(OWN) + n_shared,)),
                dma((group,)), dma((group,)), dma((group,)), dma((group,)), dma((group,)), dma((group,)),
                dma, dma, pltpu.SemaphoreType.REGULAR((3,)),
            ],
            compiler_params=pltpu.CompilerParams(
                collective_id=0, has_side_effects=True, vmem_limit_bytes=60 * 2**20),
        )(hidden, norm_w, embedding, draft_ids)
        return pl.pallas_call(
            functools.partial(combine_kernel, npos),
            out_shape=[jax.ShapeDtypeStruct((1, npos), jnp.float32)] * 2,
            in_specs=[pl.BlockSpec(memory_space=pltpu.VMEM)],
            out_specs=[pl.BlockSpec(memory_space=pltpu.VMEM)] * 2,
            compiler_params=pltpu.CompilerParams(vmem_limit_bytes=2**20),
        )(got)

    return jax.shard_map(
        local_part, mesh=mesh,
        in_specs=(P("dp", None, None), P(None), P("tp", None), P("dp", None)),
        out_specs=(P("dp", None), P("dp", None)), check_vma=False)
```

```python
import functools

import jax
import jax.numpy as jnp
from jax import lax
from jax.experimental import pallas as pl
from jax.experimental.pallas import tpu as pltpu
from jax.sharding import PartitionSpec as P

EPS = 1e-6
MESH = pl.DeviceIdType.MESH
LANES = 128
HALVES = 2
PARTS = 2
SHARE = 4
OWN = (1024, 1536)
CHUNK = 1024
UNIT = 128
EARLY = 3
BLOCKS = (1, 2, 2)
FIRST_LOADS = 1
SECOND_LOADS = 5


def shared_chunks(rows):
    sizes = [CHUNK] * (rows // CHUNK)
    return sizes + ([rows % CHUNK] if rows % CHUNK else [])


def cut(lo, n):
    return [(lo + u, min(UNIT, n - u)) for u in range(0, n, UNIT)]


def dot_rows(e, h):
    n = e.shape[0] // PARTS
    return [
        lax.dot_general(e[m * n:(m + 1) * n, :], h, (((1,), (1,)), ((), ())), preferred_element_type=jnp.float32)
        for m in range(PARTS)
    ]


def fold(z, first, want, state):
    n, width = z.shape
    z = z.reshape(n // 8, 8, width)
    row = lax.broadcasted_iota(jnp.int32, z.shape, 0) * 8 + first
    pick = jnp.sum(jnp.where(row == want[None], z, 0.0), axis=0)
    top = jnp.max(z, axis=0)
    if state is not None:
        top = jnp.maximum(top, state[0])
    e = jnp.exp(z - top[None])
    total = jnp.sum(e, axis=0)
    weighted = jnp.sum(e * z, axis=0)
    if state is not None:
        fade = jnp.exp(state[0] - top)
        total, weighted, pick = total + state[1] * fade, weighted + state[2] * fade, pick + state[3]
    return top, total, weighted, pick


def head_kernel(
    group, tp, hid_hbm, w_hbm, emb_hbm, ids_hbm, got_ref,
    hid_v, w_v, ids_v, hx, ids_x, h_own, h_all, ebuf, zo, zs, sbuf, rbuf,
    in_sem, esem, h_send, h_recv, f_send, f_recv, id_send, id_recv, s_send, s_recv, token,
):
    npos, depth = hid_v.shape
    half = depth // HALVES
    shard = emb_hbm.shape[0]
    n_own = sum(OWN)
    rows = (shard - n_own) // group
    shared = shared_chunks(rows)
    nsrc = group * tp
    width = group * npos

    dp_me = lax.axis_index("dp")
    tp_me = lax.axis_index("tp")
    q = lax.rem(dp_me, group)
    base = dp_me - q
    c = lax.rem(tp_me, 2)
    sibling = tp_me + 1 - 2 * c
    me = q * tp + tp_me

    def member(r):
        if group == 4:
            a, b = q // 2, lax.rem(q, 2)
            return lax.rem(a + r // 2, 2) * 2 + lax.rem(b + r % 2, 2)
        return lax.rem(q + r, group)

    others = tuple(range(group - 1, 0, -1))

    small = [
        pltpu.make_async_copy(hid_hbm.at[0], hid_v, in_sem.at[0]),
        pltpu.make_async_copy(w_hbm, w_v, in_sem.at[1]),
        pltpu.make_async_copy(ids_hbm, ids_v, in_sem.at[2]),
    ]
    for copy in small:
        copy.start()
    loads, spans, at = [], [], 0
    for j, n in enumerate(OWN + tuple(shared)):
        src = at if j < len(OWN) else at + q * rows
        loads.append(pltpu.make_async_copy(
            emb_hbm.at[pl.ds(src, n)], ebuf.at[pl.ds(at, n)], esem.at[j]))
        spans.append((at, n))
        at += n

    for copy in loads[:FIRST_LOADS]:
        copy.start()

    barrier = pltpu.get_barrier_semaphore()
    beside = (lax.rem(tp_me + 2, tp), lax.rem(tp_me + tp - 2, tp))
    near = [(base + member(r), tp_me) for r in others] + [(dp_me, sibling)] + [(dp_me, t) for t in beside]
    for device in near:
        pl.semaphore_signal(barrier, inc=1, device_id=device, device_id_type=MESH)

    small[0].wait()
    small[1].wait()
    x = hid_v[...].astype(jnp.float32)
    scale = lax.rsqrt(jnp.mean(x * x, axis=-1, keepdims=True) + EPS)
    h = (x * scale * (1.0 + w_v[...].astype(jnp.float32).reshape(1, depth))).astype(jnp.bfloat16)
    h32 = h.astype(jnp.float32)
    for s in range(HALVES):
        hx[q, s] = h32[:, s * half:(s + 1) * half]
    h_own[...] = h
    small[2].wait()
    ids_x[q] = jnp.concatenate([ids_v[...], jnp.full((1, LANES - npos), -1, jnp.int32)], axis=1)

    pl.semaphore_wait(barrier, len(near))

    direct, ident, forward = {}, {}, {}
    for r in others:
        direct[r] = pltpu.make_async_remote_copy(
            src_ref=hx.at[q, c], dst_ref=hx.at[q, c], send_sem=h_send.at[r], recv_sem=h_recv.at[r],
            device_id=(base + member(r), tp_me), device_id_type=MESH)
        direct[r].start()
    for r in others:
        ident[r] = pltpu.make_async_remote_copy(
            src_ref=ids_x.at[q], dst_ref=ids_x.at[q], send_sem=id_send.at[r], recv_sem=id_recv.at[r],
            device_id=(base + member(r), tp_me), device_id_type=MESH)
        ident[r].start()
    for copy in loads[FIRST_LOADS:SECOND_LOADS]:
        copy.start()

    def tell(k):
        for device in near[-2:] if k < 2 else near[-3:-2]:
            pl.semaphore_signal(token.at[k], inc=1, device_id=device, device_id_type=MESH)

    def hear(k):
        pl.semaphore_wait(token.at[k], 2 if k < 2 else 1)

    tell(0)

    def place(p, s):
        h_all[s, pl.ds(pl.multiple_of(p * npos, npos), npos), :] = hx[p, s].astype(jnp.bfloat16)

    sub = lax.broadcasted_iota(jnp.int32, (8, npos), 0)
    want_own = jnp.broadcast_to(ids_x[q][:, :npos], (8, npos)) - tp_me * shard - sub
    own = None

    def own_fold(unit, own):
        lo, n = unit
        return fold(zo[lo // UNIT, :n, :], lo, want_own, own)

    h_mine = h_own[...]
    pending = None
    for j in range(len(OWN)):
        lo, count = spans[j]
        loads[j].wait()
        for unit in cut(lo, count):
            lo, n = unit
            for m, part in enumerate(dot_rows(ebuf.at[pl.ds(lo, n)], h_mine)):
                zo[lo // UNIT, m * (n // PARTS):(m + 1) * (n // PARTS), :] = part
            if pending is not None:
                own = own_fold(pending, own)
            pending = unit
        if j == 0:
            hear(0)
            tell(1)

    for r in others:
        p = member(r)
        direct[r].wait_recv()
        forward[r] = pltpu.make_async_remote_copy(
            src_ref=hx.at[p, c], dst_ref=hx.at[p, c], send_sem=f_send.at[r], recv_sem=f_recv.at[r],
            device_id=(dp_me, sibling), device_id_type=MESH)
        forward[r].start()
    for copy in loads[SECOND_LOADS:]:
        copy.start()
    hear(1)
    tell(2)
    for r in others:
        ident[r].wait_recv()
        place(member(r), c)
    for s in range(HALVES):
        place(q, s)

    lane = lax.broadcasted_iota(jnp.int32, (8, LANES), 1)
    want = jnp.full((8, LANES), -1, jnp.int32)
    for p in range(group):
        moved = jnp.broadcast_to(ids_x[p], (8, LANES))
        if p:
            moved = pltpu.roll(moved, p * npos, 1)
        want = jnp.where((lane >= p * npos) & (lane < (p + 1) * npos), moved, want)
    first_row = tp_me * shard + n_own + q * rows
    want = (want - first_row - lax.broadcasted_iota(jnp.int32, (8, LANES), 0))[:, :width]

    units = [cut(*span) for span in spans[len(OWN):]]
    order = [unit for chunk in units for unit in chunk]

    def keep(unit, col, width_in, h, add):
        lo, n = unit
        for m, part in enumerate(dot_rows(ebuf.at[pl.ds(lo, n), pl.ds(col, width_in)], h)):
            at = slice(m * (n // PARTS), (m + 1) * (n // PARTS))
            u = order.index(unit)
            zs[u, at, :] = part + zs[u, at, :] if add else part

    def shared_fold(unit, state):
        lo, n = unit
        return fold(zs[order.index(unit), :n, :], lo - n_own, want, state)

    for j in range(EARLY):
        loads[len(OWN) + j].wait()
        for unit in units[j]:
            keep(unit, pl.multiple_of(c * half, half), half, h_all[c], False)
        if j == 0:
            own = own_fold(pending, own)

    mine = (lane >= q * npos) & (lane < (q + 1) * npos)

    def spread(v, other):
        v = jnp.concatenate([v, jnp.zeros((8, LANES - npos), jnp.float32)], axis=1)
        return jnp.where(mine, pltpu.roll(v, q * npos, 1), other)[:, :width]

    state = tuple(spread(v, other) for v, other in zip(own, (-jnp.inf, 0.0, 0.0, 0.0)))

    for r in others:
        forward[r].wait_recv()
        place(member(r), 1 - c)
    hear(2)
    pending = None
    for j in range(EARLY):
        for unit in units[j]:
            keep(unit, pl.multiple_of((1 - c) * half, half), half, h_all[1 - c], True)
            if pending is not None:
                state = shared_fold(pending, state)
            pending = unit

    h_pos = jnp.concatenate([h_all[s] for s in range(HALVES)], axis=1)
    at = EARLY
    for size in BLOCKS:
        end = min(at + size, len(shared))
        for j in range(at, end):
            loads[len(OWN) + j].wait()
        for j in range(at, end):
            for unit in units[j]:
                keep(unit, 0, depth, h_pos, False)
                state = shared_fold(pending, state)
                pending = unit
        at = end
    state = shared_fold(pending, state)

    top8, total8, weighted8, pick8 = (
        jnp.concatenate([v, jnp.zeros((8, LANES - width), jnp.float32)], axis=1) for v in state)
    top = jnp.max(top8, axis=0, keepdims=True)
    fade = jnp.exp(top8 - top)
    full = lambda v: jnp.broadcast_to(v, (8, LANES))
    top = full(top)
    total = full(jnp.sum(total8 * fade, axis=0, keepdims=True))
    weighted = full(jnp.sum(weighted8 * fade, axis=0, keepdims=True))
    pick = full(jnp.sum(pick8, axis=0, keepdims=True))
    for p in range(group):
        message = jnp.zeros((8, LANES), jnp.float32)
        for at, v in ((0, top), (1, top), (4, total), (5, weighted), (6, pick)):
            shift = (at * npos - p * npos) % LANES
            moved = pltpu.roll(v, shift, 1) if shift else v
            message = jnp.where((lane >= at * npos) & (lane < (at + 1) * npos), moved, message)
        sbuf[p] = message[:1]

    far_first = (tp // 2, tp // 2 + 1) + tuple(t for t in range(tp) if t not in (tp // 2, tp // 2 + 1))
    for r in others + (0,):
        for t in far_first:
            if r or t:
                pltpu.make_async_remote_copy(
                    src_ref=sbuf.at[member(r)], dst_ref=rbuf.at[me], send_sem=s_send, recv_sem=s_recv,
                    device_id=(base + member(r), lax.rem(tp_me + t, tp)), device_id_type=MESH).start()
    rbuf[me] = sbuf[q]
    for copies in (direct, ident, forward):
        for copy in copies.values():
            copy.wait_send()
    everyone = pltpu.make_async_remote_copy(
        src_ref=rbuf.at[pl.ds(0, nsrc - 1)], dst_ref=rbuf.at[pl.ds(0, nsrc - 1)], send_sem=s_send, recv_sem=s_recv,
        device_id=(dp_me, tp_me), device_id_type=MESH)
    everyone.wait_recv()
    everyone.wait_send()
    got_ref[...] = rbuf[...]


def combine_kernel(npos, got_ref, lp_ref, ent_ref):
    got = got_ref[...]
    values = pltpu.roll(got, LANES // 2, 2)
    top = jnp.max(got, axis=0)
    sums = jnp.sum(jnp.exp(got - top[None]) * values, axis=0)
    total = sums[:, :npos]
    weighted = pltpu.roll(sums, LANES - npos, 1)[:, :npos]
    pick = pltpu.roll(sums, LANES - 2 * npos, 1)[:, :npos]
    log_norm = top[:, :npos] + jnp.log(total)
    lp_ref[...] = pick - log_norm
    ent_ref[...] = log_norm - weighted / total


def solution(mesh):
    tp = mesh.shape["tp"]
    group = next(n for n in (SHARE, 2, 1) if mesh.shape["dp"] % n == 0)

    def local_part(hidden, norm_w, embedding, draft_ids):
        npos, depth = hidden.shape[1:]
        shard = embedding.shape[0]
        rows = (shard - sum(OWN)) // group
        half = depth // HALVES
        n_shared = len(shared_chunks(rows))
        n_units = sum(-(-n // UNIT) for n in shared_chunks(rows))
        any_spec = pl.BlockSpec(memory_space=pl.ANY)
        dma = pltpu.SemaphoreType.DMA
        got = pl.pallas_call(
            functools.partial(head_kernel, group, tp),
            out_shape=pltpu.VMEM((group * tp, 1, LANES), jnp.float32),
            in_specs=[any_spec] * 4,
            out_specs=pl.BlockSpec(memory_space=pltpu.VMEM),
            scratch_shapes=[
                pltpu.VMEM((npos, depth), jnp.bfloat16),
                pltpu.VMEM((depth,), jnp.bfloat16),
                pltpu.VMEM((1, npos), jnp.int32),
                pltpu.VMEM((group, HALVES, npos, half), jnp.float32),
                pltpu.VMEM((group, 1, LANES), jnp.int32),
                pltpu.VMEM((npos, depth), jnp.bfloat16),
                pltpu.VMEM((HALVES, group * npos, half), jnp.bfloat16),
                pltpu.VMEM((sum(OWN) + rows, depth), jnp.bfloat16),
                pltpu.VMEM((sum(OWN) // UNIT, UNIT, npos), jnp.float32),
                pltpu.VMEM((n_units, UNIT, group * npos), jnp.float32),
                pltpu.VMEM((group, 1, LANES), jnp.float32),
                pltpu.VMEM((group * tp, 1, LANES), jnp.float32),
                dma((3,)), dma((len(OWN) + n_shared,)),
                dma((group,)), dma((group,)), dma((group,)), dma((group,)), dma((group,)), dma((group,)),
                dma, dma, pltpu.SemaphoreType.REGULAR((3,)),
            ],
            compiler_params=pltpu.CompilerParams(
                collective_id=0, has_side_effects=True, vmem_limit_bytes=60 * 2**20),
        )(hidden, norm_w, embedding, draft_ids)
        return pl.pallas_call(
            functools.partial(combine_kernel, npos),
            out_shape=[jax.ShapeDtypeStruct((1, npos), jnp.float32)] * 2,
            in_specs=[pl.BlockSpec(memory_space=pltpu.VMEM)],
            out_specs=[pl.BlockSpec(memory_space=pltpu.VMEM)] * 2,
            compiler_params=pltpu.CompilerParams(vmem_limit_bytes=2**20),
        )(got)

    return jax.shard_map(
        local_part, mesh=mesh,
        in_specs=(P("dp", None, None), P(None), P("tp", None), P("dp", None)),
        out_specs=(P("dp", None), P("dp", None)), check_vma=False)
```

```python
import functools

import jax
import jax.numpy as jnp
from jax import lax
from jax.experimental import pallas as pl
from jax.experimental.pallas import tpu as pltpu
from jax.sharding import PartitionSpec as P

EPS = 1e-6
MESH = pl.DeviceIdType.MESH
LANES = 128
HALVES = 2
PARTS = 2
SHARE = 4
OWN = (1024, 768)
CHUNK = 1024
UNIT = 128
EARLY = 2
BLOCKS = (2, 2, 2)
FIRST_LOADS = 1
SECOND_LOADS = 5


def shared_chunks(rows):
    sizes = [CHUNK] * (rows // CHUNK)
    return sizes + ([rows % CHUNK] if rows % CHUNK else [])


def cut(lo, n):
    return [(lo + u, min(UNIT, n - u)) for u in range(0, n, UNIT)]


def dot_rows(e, h):
    n = e.shape[0] // PARTS
    return [
        lax.dot_general(e[m * n:(m + 1) * n, :], h, (((1,), (1,)), ((), ())), preferred_element_type=jnp.float32)
        for m in range(PARTS)
    ]


def fold(z, first, want, state):
    n, width = z.shape
    z = z.reshape(n // 8, 8, width)
    row = lax.broadcasted_iota(jnp.int32, z.shape, 0) * 8 + first
    pick = jnp.sum(jnp.where(row == want[None], z, 0.0), axis=0)
    top = jnp.max(z, axis=0)
    if state is not None:
        top = jnp.maximum(top, state[0])
    e = jnp.exp(z - top[None])
    total = jnp.sum(e, axis=0)
    weighted = jnp.sum(e * z, axis=0)
    if state is not None:
        fade = jnp.exp(state[0] - top)
        total, weighted, pick = total + state[1] * fade, weighted + state[2] * fade, pick + state[3]
    return top, total, weighted, pick


def head_kernel(
    group, tp, hid_hbm, w_hbm, emb_hbm, ids_hbm, got_ref,
    hid_v, w_v, ids_v, hx, ids_x, h_own, h_all, ebuf, zo, zs, sbuf, rbuf,
    in_sem, esem, h_send, h_recv, f_send, f_recv, id_send, id_recv, s_send, s_recv, token,
):
    npos, depth = hid_v.shape
    half = depth // HALVES
    shard = emb_hbm.shape[0]
    n_own = sum(OWN)
    rows = (shard - n_own) // group
    shared = shared_chunks(rows)
    nsrc = group * tp
    width = group * npos

    dp_me = lax.axis_index("dp")
    tp_me = lax.axis_index("tp")
    q = lax.rem(dp_me, group)
    base = dp_me - q
    c = lax.rem(tp_me, 2)
    sibling = tp_me + 1 - 2 * c
    me = q * tp + tp_me

    def member(r):
        if group == 4:
            a, b = q // 2, lax.rem(q, 2)
            return lax.rem(a + r // 2, 2) * 2 + lax.rem(b + r % 2, 2)
        return lax.rem(q + r, group)

    others = tuple(range(group - 1, 0, -1))
    arrival = (1, 3, 2) if group == 4 else others

    small = [
        pltpu.make_async_copy(hid_hbm.at[0], hid_v, in_sem.at[0]),
        pltpu.make_async_copy(w_hbm, w_v, in_sem.at[1]),
        pltpu.make_async_copy(ids_hbm, ids_v, in_sem.at[2]),
    ]
    for copy in small:
        copy.start()
    loads, spans, at = [], [], 0
    for j, n in enumerate(OWN + tuple(shared)):
        src = at if j < len(OWN) else at + q * rows
        loads.append(pltpu.make_async_copy(
            emb_hbm.at[pl.ds(src, n)], ebuf.at[pl.ds(at, n)], esem.at[j]))
        spans.append((at, n))
        at += n

    for copy in loads[:FIRST_LOADS]:
        copy.start()

    barrier = pltpu.get_barrier_semaphore()
    beside = (lax.rem(tp_me + 2, tp), lax.rem(tp_me + tp - 2, tp))
    near = [(base + member(r), tp_me) for r in others] + [(dp_me, sibling)] + [(dp_me, t) for t in beside]
    for device in near:
        pl.semaphore_signal(barrier, inc=1, device_id=device, device_id_type=MESH)

    small[0].wait()
    small[1].wait()
    x = hid_v[...].astype(jnp.float32)
    scale = lax.rsqrt(jnp.mean(x * x, axis=-1, keepdims=True) + EPS)
    h = (x * scale * (1.0 + w_v[...].astype(jnp.float32).reshape(1, depth))).astype(jnp.bfloat16)
    h32 = h.astype(jnp.float32)
    for s in range(HALVES):
        hx[q, s] = h32[:, s * half:(s + 1) * half]
    h_own[...] = h
    small[2].wait()
    ids_x[q] = jnp.concatenate([ids_v[...], jnp.full((1, LANES - npos), -1, jnp.int32)], axis=1)

    pl.semaphore_wait(barrier, len(near))

    direct, ident, forward = {}, {}, {}
    for r in others:
        direct[r] = pltpu.make_async_remote_copy(
            src_ref=hx.at[q, c], dst_ref=hx.at[q, c], send_sem=h_send.at[r], recv_sem=h_recv.at[r],
            device_id=(base + member(r), tp_me), device_id_type=MESH)
        direct[r].start()
    for r in others:
        ident[r] = pltpu.make_async_remote_copy(
            src_ref=ids_x.at[q], dst_ref=ids_x.at[q], send_sem=id_send.at[r], recv_sem=id_recv.at[r],
            device_id=(base + member(r), tp_me), device_id_type=MESH)
        ident[r].start()
    for copy in loads[FIRST_LOADS:SECOND_LOADS]:
        copy.start()

    def tell(k):
        for device in near[-2:] if k < 2 else near[-3:-2]:
            pl.semaphore_signal(token.at[k], inc=1, device_id=device, device_id_type=MESH)

    def hear(k):
        pl.semaphore_wait(token.at[k], 2 if k < 2 else 1)

    tell(0)

    def place(p, s):
        h_all[s, pl.ds(pl.multiple_of(p * npos, npos), npos), :] = hx[p, s].astype(jnp.bfloat16)

    sub = lax.broadcasted_iota(jnp.int32, (8, npos), 0)
    want_own = jnp.broadcast_to(ids_x[q][:, :npos], (8, npos)) - tp_me * shard - sub
    own = None

    def own_fold(unit, own):
        lo, n = unit
        return fold(zo[lo // UNIT, :n, :], lo, want_own, own)

    h_mine = h_own[...]
    pending = None
    for j in range(len(OWN)):
        lo, count = spans[j]
        loads[j].wait()
        for unit in cut(lo, count):
            lo, n = unit
            for m, part in enumerate(dot_rows(ebuf.at[pl.ds(lo, n)], h_mine)):
                zo[lo // UNIT, m * (n // PARTS):(m + 1) * (n // PARTS), :] = part
            if pending is not None:
                own = own_fold(pending, own)
            pending = unit
        if j == 0:
            hear(0)
            tell(1)

    for s in range(HALVES):
        place(q, s)
    for r in arrival:
        p = member(r)
        direct[r].wait_recv()
        forward[r] = pltpu.make_async_remote_copy(
            src_ref=hx.at[p, c], dst_ref=hx.at[p, c], send_sem=f_send.at[r], recv_sem=f_recv.at[r],
            device_id=(dp_me, sibling), device_id_type=MESH)
        forward[r].start()
        if r == arrival[-1]:
            for copy in loads[SECOND_LOADS:]:
                copy.start()
        place(p, c)
    for r in others:
        ident[r].wait_recv()

    lane = lax.broadcasted_iota(jnp.int32, (8, LANES), 1)
    want = jnp.full((8, LANES), -1, jnp.int32)
    for p in range(group):
        moved = jnp.broadcast_to(ids_x[p], (8, LANES))
        if p:
            moved = pltpu.roll(moved, p * npos, 1)
        want = jnp.where((lane >= p * npos) & (lane < (p + 1) * npos), moved, want)
    first_row = tp_me * shard + n_own + q * rows
    want = (want - first_row - lax.broadcasted_iota(jnp.int32, (8, LANES), 0))[:, :width]

    units = [cut(*span) for span in spans[len(OWN):]]
    order = [unit for chunk in units for unit in chunk]

    def keep(unit, col, width_in, h, add):
        lo, n = unit
        for m, part in enumerate(dot_rows(ebuf.at[pl.ds(lo, n), pl.ds(col, width_in)], h)):
            at = slice(m * (n // PARTS), (m + 1) * (n // PARTS))
            u = order.index(unit)
            zs[u, at, :] = part + zs[u, at, :] if add else part

    def shared_fold(unit, state):
        lo, n = unit
        return fold(zs[order.index(unit), :n, :], lo - n_own, want, state)

    for j in range(EARLY):
        loads[len(OWN) + j].wait()
    for j in range(EARLY):
        for unit in units[j]:
            keep(unit, pl.multiple_of(c * half, half), half, h_all[c], False)
        if j == 0:
            own = own_fold(pending, own)

    mine = (lane >= q * npos) & (lane < (q + 1) * npos)

    def spread(v, other):
        v = jnp.concatenate([v, jnp.zeros((8, LANES - npos), jnp.float32)], axis=1)
        return jnp.where(mine, pltpu.roll(v, q * npos, 1), other)[:, :width]

    state = tuple(spread(v, other) for v, other in zip(own, (-jnp.inf, 0.0, 0.0, 0.0)))

    for r in others:
        forward[r].wait_recv()
        place(member(r), 1 - c)
    hear(1)
    tell(2)
    pending = None
    for j in range(EARLY):
        for unit in units[j]:
            keep(unit, pl.multiple_of((1 - c) * half, half), half, h_all[1 - c], True)
            if pending is not None:
                state = shared_fold(pending, state)
            pending = unit

    h_pos = jnp.concatenate([h_all[s] for s in range(HALVES)], axis=1)
    at = EARLY
    for size in BLOCKS:
        end = min(at + size, len(shared))
        for j in range(at, end):
            loads[len(OWN) + j].wait()
        for j in range(at, end):
            for unit in units[j]:
                keep(unit, 0, depth, h_pos, False)
                state = shared_fold(pending, state)
                pending = unit
        if at == EARLY:
            hear(2)
        at = end
    state = shared_fold(pending, state)

    top8, total8, weighted8, pick8 = (
        jnp.concatenate([v, jnp.zeros((8, LANES - width), jnp.float32)], axis=1) for v in state)
    top = jnp.max(top8, axis=0, keepdims=True)
    fade = jnp.exp(top8 - top)
    full = lambda v: jnp.broadcast_to(v, (8, LANES))
    top = full(top)
    total = full(jnp.sum(total8 * fade, axis=0, keepdims=True))
    weighted = full(jnp.sum(weighted8 * fade, axis=0, keepdims=True))
    pick = full(jnp.sum(pick8, axis=0, keepdims=True))
    for p in range(group):
        message = jnp.zeros((8, LANES), jnp.float32)
        for at, v in ((0, top), (1, top), (4, total), (5, weighted), (6, pick)):
            shift = (at * npos - p * npos) % LANES
            moved = pltpu.roll(v, shift, 1) if shift else v
            message = jnp.where((lane >= at * npos) & (lane < (at + 1) * npos), moved, message)
        sbuf[p] = message[:1]

    far_first = (tp // 2, tp // 2 + 1) + tuple(t for t in range(tp) if t not in (tp // 2, tp // 2 + 1))
    for r in others + (0,):
        for t in far_first:
            if r or t:
                pltpu.make_async_remote_copy(
                    src_ref=sbuf.at[member(r)], dst_ref=rbuf.at[me], send_sem=s_send, recv_sem=s_recv,
                    device_id=(base + member(r), lax.rem(tp_me + t, tp)), device_id_type=MESH).start()
    rbuf[me] = sbuf[q]
    for copies in (direct, ident, forward):
        for copy in copies.values():
            copy.wait_send()
    everyone = pltpu.make_async_remote_copy(
        src_ref=rbuf.at[pl.ds(0, nsrc - 1)], dst_ref=rbuf.at[pl.ds(0, nsrc - 1)], send_sem=s_send, recv_sem=s_recv,
        device_id=(dp_me, tp_me), device_id_type=MESH)
    everyone.wait_recv()
    everyone.wait_send()
    got_ref[...] = rbuf[...]


def combine_kernel(npos, got_ref, lp_ref, ent_ref):
    got = got_ref[...]
    values = pltpu.roll(got, LANES // 2, 2)
    top = jnp.max(got, axis=0)
    sums = jnp.sum(jnp.exp(got - top[None]) * values, axis=0)
    total = sums[:, :npos]
    weighted = pltpu.roll(sums, LANES - npos, 1)[:, :npos]
    pick = pltpu.roll(sums, LANES - 2 * npos, 1)[:, :npos]
    log_norm = top[:, :npos] + jnp.log(total)
    lp_ref[...] = pick - log_norm
    ent_ref[...] = log_norm - weighted / total


def solution(mesh):
    tp = mesh.shape["tp"]
    group = next(n for n in (SHARE, 2, 1) if mesh.shape["dp"] % n == 0)

    def local_part(hidden, norm_w, embedding, draft_ids):
        npos, depth = hidden.shape[1:]
        shard = embedding.shape[0]
        rows = (shard - sum(OWN)) // group
        half = depth // HALVES
        n_shared = len(shared_chunks(rows))
        n_units = sum(-(-n // UNIT) for n in shared_chunks(rows))
        any_spec = pl.BlockSpec(memory_space=pl.ANY)
        dma = pltpu.SemaphoreType.DMA
        got = pl.pallas_call(
            functools.partial(head_kernel, group, tp),
            out_shape=pltpu.VMEM((group * tp, 1, LANES), jnp.float32),
            in_specs=[any_spec] * 4,
            out_specs=pl.BlockSpec(memory_space=pltpu.VMEM),
            scratch_shapes=[
                pltpu.VMEM((npos, depth), jnp.bfloat16),
                pltpu.VMEM((depth,), jnp.bfloat16),
                pltpu.VMEM((1, npos), jnp.int32),
                pltpu.VMEM((group, HALVES, npos, half), jnp.float32),
                pltpu.VMEM((group, 1, LANES), jnp.int32),
                pltpu.VMEM((npos, depth), jnp.bfloat16),
                pltpu.VMEM((HALVES, group * npos, half), jnp.bfloat16),
                pltpu.VMEM((sum(OWN) + rows, depth), jnp.bfloat16),
                pltpu.VMEM((sum(OWN) // UNIT, UNIT, npos), jnp.float32),
                pltpu.VMEM((n_units, UNIT, group * npos), jnp.float32),
                pltpu.VMEM((group, 1, LANES), jnp.float32),
                pltpu.VMEM((group * tp, 1, LANES), jnp.float32),
                dma((3,)), dma((len(OWN) + n_shared,)),
                dma((group,)), dma((group,)), dma((group,)), dma((group,)), dma((group,)), dma((group,)),
                dma, dma, pltpu.SemaphoreType.REGULAR((3,)),
            ],
            compiler_params=pltpu.CompilerParams(
                collective_id=0, has_side_effects=True, vmem_limit_bytes=60 * 2**20),
        )(hidden, norm_w, embedding, draft_ids)
        return pl.pallas_call(
            functools.partial(combine_kernel, npos),
            out_shape=[jax.ShapeDtypeStruct((1, npos), jnp.float32)] * 2,
            in_specs=[pl.BlockSpec(memory_space=pltpu.VMEM)],
            out_specs=[pl.BlockSpec(memory_space=pltpu.VMEM)] * 2,
            compiler_params=pltpu.CompilerParams(vmem_limit_bytes=2**20),
        )(got)

    return jax.shard_map(
        local_part, mesh=mesh,
        in_specs=(P("dp", None, None), P(None), P("tp", None), P("dp", None)),
        out_specs=(P("dp", None), P("dp", None)), check_vma=False)
```

```python
import functools

import jax
import jax.numpy as jnp
from jax import lax
from jax.experimental import pallas as pl
from jax.experimental.pallas import tpu as pltpu
from jax.sharding import PartitionSpec as P

EPS = 1e-6
MESH = pl.DeviceIdType.MESH
LANES = 128
HALVES = 2
PARTS = 2
SHARE = 4
OWN = (1024, 1024)
CHUNK = 1024
UNIT = 128
EARLY = 2
BLOCKS = (1, 2, 3)
FIRST_LOADS = 1
SECOND_LOADS = 5


def shared_chunks(rows):
    sizes = [CHUNK] * (rows // CHUNK)
    return sizes + ([rows % CHUNK] if rows % CHUNK else [])


def cut(lo, n):
    return [(lo + u, min(UNIT, n - u)) for u in range(0, n, UNIT)]


def dot_rows(e, h):
    n = e.shape[0] // PARTS
    return [
        lax.dot_general(e[m * n:(m + 1) * n, :], h, (((1,), (1,)), ((), ())), preferred_element_type=jnp.float32)
        for m in range(PARTS)
    ]


def fold(z, first, want, state):
    n, width = z.shape
    z = z.reshape(n // 8, 8, width)
    row = lax.broadcasted_iota(jnp.int32, z.shape, 0) * 8 + first
    pick = jnp.sum(jnp.where(row == want[None], z, 0.0), axis=0)
    top = jnp.max(z, axis=0)
    if state is not None:
        top = jnp.maximum(top, state[0])
    e = jnp.exp(z - top[None])
    total = jnp.sum(e, axis=0)
    weighted = jnp.sum(e * z, axis=0)
    if state is not None:
        fade = jnp.exp(state[0] - top)
        total, weighted, pick = total + state[1] * fade, weighted + state[2] * fade, pick + state[3]
    return top, total, weighted, pick


def head_kernel(
    group, tp, hid_hbm, w_hbm, emb_hbm, ids_hbm, got_ref,
    hid_v, w_v, ids_v, hx, ids_x, h_own, h_all, ebuf, zo, zs, sbuf, rbuf,
    in_sem, esem, h_send, h_recv, f_send, f_recv, id_send, id_recv, s_send, s_recv, token,
):
    npos, depth = hid_v.shape
    half = depth // HALVES
    shard = emb_hbm.shape[0]
    n_own = sum(OWN)
    rows = (shard - n_own) // group
    shared = shared_chunks(rows)
    nsrc = group * tp
    width = group * npos

    dp_me = lax.axis_index("dp")
    tp_me = lax.axis_index("tp")
    q = lax.rem(dp_me, group)
    base = dp_me - q
    c = lax.rem(tp_me, 2)
    sibling = tp_me + 1 - 2 * c
    me = q * tp + tp_me

    def member(r):
        if group == 4:
            a, b = q // 2, lax.rem(q, 2)
            return lax.rem(a + r // 2, 2) * 2 + lax.rem(b + r % 2, 2)
        return lax.rem(q + r, group)

    others = tuple(range(group - 1, 0, -1))
    arrival = (1, 3, 2) if group == 4 else others

    small = [
        pltpu.make_async_copy(hid_hbm.at[0], hid_v, in_sem.at[0]),
        pltpu.make_async_copy(w_hbm, w_v, in_sem.at[1]),
        pltpu.make_async_copy(ids_hbm, ids_v, in_sem.at[2]),
    ]
    for copy in small:
        copy.start()
    loads, spans, at = [], [], 0
    for j, n in enumerate(OWN + tuple(shared)):
        src = at if j < len(OWN) else at + q * rows
        loads.append(pltpu.make_async_copy(
            emb_hbm.at[pl.ds(src, n)], ebuf.at[pl.ds(at, n)], esem.at[j]))
        spans.append((at, n))
        at += n

    for copy in loads[:FIRST_LOADS]:
        copy.start()

    barrier = pltpu.get_barrier_semaphore()
    beside = (lax.rem(tp_me + 2, tp), lax.rem(tp_me + tp - 2, tp))
    near = [(base + member(r), tp_me) for r in others] + [(dp_me, sibling)] + [(dp_me, t) for t in beside]
    for device in near:
        pl.semaphore_signal(barrier, inc=1, device_id=device, device_id_type=MESH)

    small[0].wait()
    small[1].wait()
    x = hid_v[...].astype(jnp.float32)
    scale = lax.rsqrt(jnp.mean(x * x, axis=-1, keepdims=True) + EPS)
    h = (x * scale * (1.0 + w_v[...].astype(jnp.float32).reshape(1, depth))).astype(jnp.bfloat16)
    h32 = h.astype(jnp.float32)
    for s in range(HALVES):
        hx[q, s] = h32[:, s * half:(s + 1) * half]
    h_own[...] = h
    small[2].wait()
    ids_x[q] = jnp.concatenate([ids_v[...], jnp.full((1, LANES - npos), -1, jnp.int32)], axis=1)

    pl.semaphore_wait(barrier, len(near))

    direct, ident, forward = {}, {}, {}
    for r in others:
        direct[r] = pltpu.make_async_remote_copy(
            src_ref=hx.at[q, c], dst_ref=hx.at[q, c], send_sem=h_send.at[r], recv_sem=h_recv.at[r],
            device_id=(base + member(r), tp_me), device_id_type=MESH)
        direct[r].start()
    for r in others:
        ident[r] = pltpu.make_async_remote_copy(
            src_ref=ids_x.at[q], dst_ref=ids_x.at[q], send_sem=id_send.at[r], recv_sem=id_recv.at[r],
            device_id=(base + member(r), tp_me), device_id_type=MESH)
        ident[r].start()
    for copy in loads[FIRST_LOADS:SECOND_LOADS]:
        copy.start()

    def tell(k):
        for device in near[-2:] if k < 2 else near[-3:-2]:
            pl.semaphore_signal(token.at[k], inc=1, device_id=device, device_id_type=MESH)

    def hear(k):
        pl.semaphore_wait(token.at[k], 2 if k < 2 else 1)

    tell(0)

    def place(p, s):
        h_all[s, pl.ds(pl.multiple_of(p * npos, npos), npos), :] = hx[p, s].astype(jnp.bfloat16)

    sub = lax.broadcasted_iota(jnp.int32, (8, npos), 0)
    want_own = jnp.broadcast_to(ids_x[q][:, :npos], (8, npos)) - tp_me * shard - sub
    own = None

    def own_fold(unit, own):
        lo, n = unit
        return fold(zo[lo // UNIT, :n, :], lo, want_own, own)

    h_mine = h_own[...]
    pending = None
    for j in range(len(OWN)):
        lo, count = spans[j]
        loads[j].wait()
        for unit in cut(lo, count):
            lo, n = unit
            for m, part in enumerate(dot_rows(ebuf.at[pl.ds(lo, n)], h_mine)):
                zo[lo // UNIT, m * (n // PARTS):(m + 1) * (n // PARTS), :] = part
            if pending is not None:
                own = own_fold(pending, own)
            pending = unit
        if j == 0:
            hear(0)
            tell(1)

    for s in range(HALVES):
        place(q, s)
    for r in arrival:
        p = member(r)
        direct[r].wait_recv()
        forward[r] = pltpu.make_async_remote_copy(
            src_ref=hx.at[p, c], dst_ref=hx.at[p, c], send_sem=f_send.at[r], recv_sem=f_recv.at[r],
            device_id=(dp_me, sibling), device_id_type=MESH)
        forward[r].start()
        if r == arrival[-1]:
            for copy in loads[SECOND_LOADS:]:
                copy.start()
        place(p, c)
    for r in others:
        ident[r].wait_recv()

    lane = lax.broadcasted_iota(jnp.int32, (8, LANES), 1)
    want = jnp.full((8, LANES), -1, jnp.int32)
    for p in range(group):
        moved = jnp.broadcast_to(ids_x[p], (8, LANES))
        if p:
            moved = pltpu.roll(moved, p * npos, 1)
        want = jnp.where((lane >= p * npos) & (lane < (p + 1) * npos), moved, want)
    first_row = tp_me * shard + n_own + q * rows
    want = (want - first_row - lax.broadcasted_iota(jnp.int32, (8, LANES), 0))[:, :width]

    units = [cut(*span) for span in spans[len(OWN):]]
    order = [unit for chunk in units for unit in chunk]

    def keep(unit, col, width_in, h, add):
        lo, n = unit
        for m, part in enumerate(dot_rows(ebuf.at[pl.ds(lo, n), pl.ds(col, width_in)], h)):
            at = slice(m * (n // PARTS), (m + 1) * (n // PARTS))
            u = order.index(unit)
            zs[u, at, :] = part + zs[u, at, :] if add else part

    def shared_fold(unit, state):
        lo, n = unit
        return fold(zs[order.index(unit), :n, :], lo - n_own, want, state)

    for j in range(EARLY):
        loads[len(OWN) + j].wait()
    for j in range(EARLY):
        for unit in units[j]:
            keep(unit, pl.multiple_of(c * half, half), half, h_all[c], False)
        if j == 0:
            own = own_fold(pending, own)

    mine = (lane >= q * npos) & (lane < (q + 1) * npos)

    def spread(v, other):
        v = jnp.concatenate([v, jnp.zeros((8, LANES - npos), jnp.float32)], axis=1)
        return jnp.where(mine, pltpu.roll(v, q * npos, 1), other)[:, :width]

    state = tuple(spread(v, other) for v, other in zip(own, (-jnp.inf, 0.0, 0.0, 0.0)))

    for r in others:
        forward[r].wait_recv()
        place(member(r), 1 - c)
    hear(1)
    tell(2)
    for j in range(EARLY, EARLY + BLOCKS[0]):
        loads[len(OWN) + j].wait()
    pending = None
    for j in range(EARLY):
        for unit in units[j]:
            keep(unit, pl.multiple_of((1 - c) * half, half), half, h_all[1 - c], True)
            if pending is not None:
                state = shared_fold(pending, state)
            pending = unit

    h_pos = jnp.concatenate([h_all[s] for s in range(HALVES)], axis=1)
    at = EARLY
    for size in BLOCKS:
        end = min(at + size, len(shared))
        for j in range(max(at, EARLY + BLOCKS[0]), end):
            loads[len(OWN) + j].wait()
        for j in range(at, end):
            for unit in units[j]:
                keep(unit, 0, depth, h_pos, False)
                state = shared_fold(pending, state)
                pending = unit
        if at > EARLY and end < len(shared):
            hear(2)
        at = end
    state = shared_fold(pending, state)

    top8, total8, weighted8, pick8 = (
        jnp.concatenate([v, jnp.zeros((8, LANES - width), jnp.float32)], axis=1) for v in state)
    top = jnp.max(top8, axis=0, keepdims=True)
    fade = jnp.exp(top8 - top)
    full = lambda v: jnp.broadcast_to(v, (8, LANES))
    top = full(top)
    total = full(jnp.sum(total8 * fade, axis=0, keepdims=True))
    weighted = full(jnp.sum(weighted8 * fade, axis=0, keepdims=True))
    pick = full(jnp.sum(pick8, axis=0, keepdims=True))
    for p in range(group):
        message = jnp.zeros((8, LANES), jnp.float32)
        for at, v in ((0, top), (1, top), (4, total), (5, weighted), (6, pick)):
            shift = (at * npos - p * npos) % LANES
            moved = pltpu.roll(v, shift, 1) if shift else v
            message = jnp.where((lane >= at * npos) & (lane < (at + 1) * npos), moved, message)
        sbuf[p] = message[:1]

    far_first = (tp // 2, tp // 2 + 1) + tuple(t for t in range(tp) if t not in (tp // 2, tp // 2 + 1))
    for r in others + (0,):
        for t in far_first:
            if r or t:
                pltpu.make_async_remote_copy(
                    src_ref=sbuf.at[member(r)], dst_ref=rbuf.at[me], send_sem=s_send, recv_sem=s_recv,
                    device_id=(base + member(r), lax.rem(tp_me + t, tp)), device_id_type=MESH).start()
    rbuf[me] = sbuf[q]
    for copies in (direct, ident, forward):
        for copy in copies.values():
            copy.wait_send()
    everyone = pltpu.make_async_remote_copy(
        src_ref=rbuf.at[pl.ds(0, nsrc - 1)], dst_ref=rbuf.at[pl.ds(0, nsrc - 1)], send_sem=s_send, recv_sem=s_recv,
        device_id=(dp_me, tp_me), device_id_type=MESH)
    everyone.wait_recv()
    everyone.wait_send()
    got_ref[...] = rbuf[...]


def combine_kernel(npos, got_ref, lp_ref, ent_ref):
    got = got_ref[...]
    values = pltpu.roll(got, LANES // 2, 2)
    top = jnp.max(got, axis=0)
    sums = jnp.sum(jnp.exp(got - top[None]) * values, axis=0)
    total = sums[:, :npos]
    weighted = pltpu.roll(sums, LANES - npos, 1)[:, :npos]
    pick = pltpu.roll(sums, LANES - 2 * npos, 1)[:, :npos]
    log_norm = top[:, :npos] + jnp.log(total)
    lp_ref[...] = pick - log_norm
    ent_ref[...] = log_norm - weighted / total


def solution(mesh):
    tp = mesh.shape["tp"]
    group = next(n for n in (SHARE, 2, 1) if mesh.shape["dp"] % n == 0)

    def local_part(hidden, norm_w, embedding, draft_ids):
        npos, depth = hidden.shape[1:]
        shard = embedding.shape[0]
        rows = (shard - sum(OWN)) // group
        half = depth // HALVES
        n_shared = len(shared_chunks(rows))
        n_units = sum(-(-n // UNIT) for n in shared_chunks(rows))
        any_spec = pl.BlockSpec(memory_space=pl.ANY)
        dma = pltpu.SemaphoreType.DMA
        got = pl.pallas_call(
            functools.partial(head_kernel, group, tp),
            out_shape=pltpu.VMEM((group * tp, 1, LANES), jnp.float32),
            in_specs=[any_spec] * 4,
            out_specs=pl.BlockSpec(memory_space=pltpu.VMEM),
            scratch_shapes=[
                pltpu.VMEM((npos, depth), jnp.bfloat16),
                pltpu.VMEM((depth,), jnp.bfloat16),
                pltpu.VMEM((1, npos), jnp.int32),
                pltpu.VMEM((group, HALVES, npos, half), jnp.float32),
                pltpu.VMEM((group, 1, LANES), jnp.int32),
                pltpu.VMEM((npos, depth), jnp.bfloat16),
                pltpu.VMEM((HALVES, group * npos, half), jnp.bfloat16),
                pltpu.VMEM((sum(OWN) + rows, depth), jnp.bfloat16),
                pltpu.VMEM((sum(OWN) // UNIT, UNIT, npos), jnp.float32),
                pltpu.VMEM((n_units, UNIT, group * npos), jnp.float32),
                pltpu.VMEM((group, 1, LANES), jnp.float32),
                pltpu.VMEM((group * tp, 1, LANES), jnp.float32),
                dma((3,)), dma((len(OWN) + n_shared,)),
                dma((group,)), dma((group,)), dma((group,)), dma((group,)), dma((group,)), dma((group,)),
                dma, dma, pltpu.SemaphoreType.REGULAR((3,)),
            ],
            compiler_params=pltpu.CompilerParams(
                collective_id=0, has_side_effects=True, vmem_limit_bytes=60 * 2**20),
        )(hidden, norm_w, embedding, draft_ids)
        return pl.pallas_call(
            functools.partial(combine_kernel, npos),
            out_shape=[jax.ShapeDtypeStruct((1, npos), jnp.float32)] * 2,
            in_specs=[pl.BlockSpec(memory_space=pltpu.VMEM)],
            out_specs=[pl.BlockSpec(memory_space=pltpu.VMEM)] * 2,
            compiler_params=pltpu.CompilerParams(vmem_limit_bytes=2**20),
        )(got)

    return jax.shard_map(
        local_part, mesh=mesh,
        in_specs=(P("dp", None, None), P(None), P("tp", None), P("dp", None)),
        out_specs=(P("dp", None), P("dp", None)), check_vma=False)
```
